32 devices in a mesh: seq: 2 (over x), dp: 16 (over z, y, core).
Axes of the slice: x: 2, y: 2, z: 4, core: 2. Of those that a mesh axis runs over, the one named last changes fastest.
Arguments:
- accept_arrays: bfloat16 [16, 256, 2048], P('dp', 'seq'), may hold values from -1.5 to 1.5
- lookup_arrays: bfloat16 [16, 256, 2048], P('dp', 'seq'), may hold values from -0.75 to 0.75
- payload_arrays: bfloat16 [16, 256, 2048], P('dp', 'seq'), may hold values from -6 to 6
- fading_exponent: bfloat16 [16, 256, 2048], P('dp', 'seq'), may hold values from -14 to 1
- self_boost: float32 [32, 64], replicated, may hold values from -3 to 3
- result_cotangent: bfloat16 [16, 256, 2048], P('dp', 'seq'), may hold values from -0.75 to 0.75
- initial_memory_matrix: float32 [2048, 64], replicated, may hold values from -12 to 12
Outputs:
- receptance_grad: bfloat16 [16, 256, 2048], P('dp', 'seq')
- lookup_cotangent: bfloat16 [16, 256, 2048], P('dp', 'seq')
- value_grad: bfloat16 [16, 256, 2048], P('dp', 'seq')
- state_grad: float32 [2048, 64], P('dp', 'seq')
The draws below stay inside these ranges and needn't reach their ends.
All inputs are finite; a program needn't handle non-finite values.
Results may differ from the reference program's by a relative error of at most 0.001.
Values sent between devices are 32-bit elements; how exact they have to be, the bound alone decides.
No kernel may reach another device: no remote copies, remote signals or barrier semaphores. Data moves between devices by JAX's collectives and lax.ppermute only.
A program may use at most 128 MiB of HBM per device.

```python
import math
import jax
import jax.numpy as jnp
from jax import lax

PARTIAL_UNITS = 32
ATTN_SIZE = 64
TOK_DEV = 128
SEQ_LEN = 256
BATCH = 16


def draw_fading_exponent(key, part):
    keys = jax.random.split(key, 7)
    shard_count = SEQ_LEN // TOK_DEV
    fast_share = 0.5
    fast = jax.random.uniform(keys[0], (PARTIAL_UNITS, 1)) < fast_share
    slow_rate = jnp.exp(jax.random.uniform(keys[1], (PARTIAL_UNITS, ATTN_SIZE), minval=math.log(0.15), maxval=math.log(0.6))) / SEQ_LEN
    fast_rate = jnp.exp(jax.random.uniform(keys[2], (PARTIAL_UNITS, ATTN_SIZE), minval=math.log(1.0 / 50.0), maxval=math.log(1.0 / 30.0)))
    base = jnp.where(fast, fast_rate, slow_rate)
    shard_factor = jnp.exp(jax.random.uniform(keys[3], (BATCH, shard_count, 1, 1, 1), minval=-0.69, maxval=0.69))
    token_factor = jnp.exp(jax.random.uniform(keys[4], (BATCH, shard_count, TOK_DEV, PARTIAL_UNITS, ATTN_SIZE), minval=-0.69, maxval=0.69))
    decay_rate = (base * shard_factor * token_factor).reshape(BATCH, SEQ_LEN, PARTIAL_UNITS, ATTN_SIZE)
    device_spots = jax.random.randint(keys[5], (BATCH, 2, 1), 0, SEQ_LEN)
    device_places = jnp.arange(SEQ_LEN, dtype=jnp.int32)[None, None, :]
    token_group = jnp.sum((device_places == device_spots).astype(jnp.float32), axis=1)
    loss_value = jax.random.uniform(keys[6], (BATCH, SEQ_LEN, PARTIAL_UNITS, 1), minval=0.2, maxval=0.5)
    decay_rate = decay_rate - token_group[:, :, None, None] * jnp.log(1.0 - loss_value)
    return jnp.log(decay_rate).reshape(BATCH, SEQ_LEN, PARTIAL_UNITS * ATTN_SIZE).astype(jnp.bfloat16)


def raised(drawn, stream_key, source, target, blocks, factor):
    def block_of(axis_at):
        return (jnp.arange(drawn.shape[axis_at]) // (drawn.shape[axis_at] // blocks)).reshape((-1,) + (1,) * (drawn.ndim - 1 - axis_at))

    near = jax.random.permutation(stream_key, blocks)[block_of(target)]
    far = (block_of(target) + blocks // 2) % blocks
    return jnp.where((block_of(source) == near) | (block_of(source) == far), factor * drawn, drawn)


def block_levels(key, shape, cuts, low, top_value):
    factor_of, own = 1.0, jax.random.fold_in(key, 6)
    for axis_at, parts in cuts:
        draws = jnp.exp(jax.random.uniform(jax.random.fold_in(own, axis_at), (parts,), jnp.float32, low / len(cuts), top_value / len(cuts)))
        factor_of = factor_of * jnp.repeat(draws, shape[axis_at] // parts).reshape([-1 if axis == axis_at else 1 for axis in range(len(shape))])
    return factor_of


def centred(key, extent, scale, limit, cuts=(), kind=jnp.bfloat16):
    drawn = scale * jax.random.normal(key, extent, jnp.float32)
    if cuts:
        drawn = drawn * block_levels(key, extent, cuts, -0.22, 0.18)
    return jnp.clip(drawn, -limit, limit).astype(kind)


def noise_with(own_key, dims, width, reach, cuts, heavy, held_as=jnp.bfloat16):
    entries = width * jax.random.normal(own_key, dims, jnp.float32)
    if cuts:
        entries = entries * block_levels(own_key, dims, cuts, -0.22, 0.18)
    return jnp.clip(raised(entries, jax.random.fold_in(own_key, 3), *heavy), -reach, reach).astype(held_as)


def setup_inputs(seed: int = 0) -> dict:
    arg_keys = jax.random.split(jax.random.key(seed), 8)
    accept_arrays = noise_with(arg_keys[0], (BATCH, SEQ_LEN, PARTIAL_UNITS * ATTN_SIZE), 0.25, 1.5, ((0, 16), (1, 2)), (0, 2, 16, 2.0))
    lookup_arrays = centred(arg_keys[1], (BATCH, SEQ_LEN, PARTIAL_UNITS * ATTN_SIZE), 0.125, 0.75, ((0, 16), (1, 2)))
    payload_arrays = centred(arg_keys[2], (BATCH, SEQ_LEN, PARTIAL_UNITS * ATTN_SIZE), 1.0, 6.0, ((0, 16), (1, 2)))
    fading_exponent = draw_fading_exponent(jax.random.fold_in(arg_keys[7], 71), 0)
    self_boost = centred(arg_keys[4], (PARTIAL_UNITS, ATTN_SIZE), 1.0, 3.0, (), jnp.float32)
    result_cotangent = centred(arg_keys[5], (BATCH, SEQ_LEN, PARTIAL_UNITS * ATTN_SIZE), 0.125, 0.75, ((0, 16), (1, 2)))
    initial_memory_matrix = centred(arg_keys[6], (PARTIAL_UNITS * ATTN_SIZE, ATTN_SIZE), 2.0, 12.0, (), jnp.float32)
    return {"accept_arrays": accept_arrays, "lookup_arrays": lookup_arrays, "payload_arrays": payload_arrays, "fading_exponent": fading_exponent, "self_boost": self_boost, "result_cotangent": result_cotangent, "initial_memory_matrix": initial_memory_matrix}


def split_heads(array):
    return array.astype(jnp.float32).reshape(BATCH, SEQ_LEN, PARTIAL_UNITS, ATTN_SIZE).transpose(1, 0, 2, 3)


def merge_heads(array):
    return array.transpose(1, 0, 2, 3).reshape(BATCH, SEQ_LEN, PARTIAL_UNITS * ATTN_SIZE).astype(jnp.bfloat16)


def reference(accept_arrays, lookup_arrays, payload_arrays, fading_exponent, self_boost, result_cotangent, initial_memory_matrix):
    accept_matrix_lines = split_heads(accept_arrays)
    lookup_matrix_slice = split_heads(lookup_arrays)
    val_rows = split_heads(payload_arrays)
    grad_rows = split_heads(result_cotangent)
    decays = jnp.exp(-jnp.exp(split_heads(fading_exponent)))
    finest_accuracy = lax.Precision.HIGHEST
    start = jnp.broadcast_to(initial_memory_matrix.astype(jnp.float32).reshape(PARTIAL_UNITS, ATTN_SIZE, ATTN_SIZE), (BATCH, PARTIAL_UNITS, ATTN_SIZE, ATTN_SIZE))

    def forward(evolving_memory, inputs):
        present_accept, present_lookup, present_payload, dec_now, present_cotangent = inputs
        scalar_dotted = jnp.sum(present_payload * present_cotangent, axis=-1, keepdims=True)
        accept_cotangent = jnp.einsum("dcpu,dcu->dcp", evolving_memory, present_cotangent, precision=finest_accuracy) + self_boost * present_lookup * scalar_dotted
        evolving_memory = dec_now[..., None] * evolving_memory + present_lookup[..., None] * present_payload[..., None, :]
        return evolving_memory, accept_cotangent

    _, rec_grads = lax.scan(forward, start, (accept_matrix_lines, lookup_matrix_slice, val_rows, decays, grad_rows))

    def backward(scan_memory, inputs):
        present_accept, present_lookup, present_payload, dec_now, present_cotangent = inputs
        scalar_dotted = jnp.sum(present_payload * present_cotangent, axis=-1, keepdims=True)
        fading_factor = jnp.sum(present_accept * self_boost * present_lookup, axis=-1, keepdims=True)
        lookup_cotangent = jnp.einsum("dcpu,dcu->dcp", scan_memory, present_payload, precision=finest_accuracy) + present_accept * self_boost * scalar_dotted
        val_grad = jnp.einsum("bhij,bhi->bhj", scan_memory, present_lookup, precision=finest_accuracy) + fading_factor * present_cotangent
        scan_memory = dec_now[..., None] * scan_memory + present_accept[..., None] * present_cotangent[..., None, :]
        return scan_memory, (lookup_cotangent, val_grad)

    zeros = jnp.zeros((BATCH, PARTIAL_UNITS, ATTN_SIZE, ATTN_SIZE), jnp.float32)
    final, (key_grads, val_grads) = lax.scan(backward, zeros, (accept_matrix_lines, lookup_matrix_slice, val_rows, decays, grad_rows), reverse=True)
    state_grad = jnp.sum(final, axis=0).reshape(PARTIAL_UNITS * ATTN_SIZE, ATTN_SIZE)
    return merge_heads(rec_grads), merge_heads(key_grads), merge_heads(val_grads), state_grad
```

```python
import jax
import jax.numpy as jnp
from jax import lax
from jax.experimental import pallas as pl
from jax.experimental.pallas import tpu as pltpu
from jax.sharding import PartitionSpec as P

LANES = 128
CHUNK = 32
BF16 = jnp.bfloat16
F32 = jnp.float32


def dot(a, b, contract=(1, 0)):
    return lax.dot_general(
        a, b, (((contract[0],), (contract[1],)), ((), ())), preferred_element_type=F32
    )


def split(x):
    hi = x.astype(BF16)
    return hi, (x - hi.astype(F32)).astype(BF16)


def triangles(toks):
    row = lax.broadcasted_iota(jnp.int32, (toks, toks), 0)
    col = lax.broadcasted_iota(jnp.int32, (toks, toks), 1)
    same = (row // CHUNK) == (col // CHUNK)
    before = jnp.where(same & (col < row), 1.0, 0.0).astype(BF16)
    after = jnp.where(same & (col > row), 1.0, 0.0).astype(BF16)
    return jnp.concatenate([before, after], 0)


def decays(fade, tri):
    toks = fade.shape[0]
    log_decay = -jnp.exp(fade.astype(F32))
    hi, lo = split(log_decay)
    sums = dot(jnp.concatenate([tri, tri], 1), jnp.concatenate([hi, lo], 0))
    prefix, suffix = sums[:toks], sums[toks:]
    totals, middles = [], []
    for c in range(toks // CHUNK):
        last = (c + 1) * CHUNK - 1
        totals.append(prefix[last : last + 1] + log_decay[last : last + 1])
        mid = c * CHUNK + CHUNK // 2
        middles.append(prefix[mid : mid + 1])
    return jnp.exp(prefix), jnp.exp(suffix), totals, middles


def spread(early, late, totals):
    chunks = len(totals)
    rows = [slice(c * CHUNK, (c + 1) * CHUNK) for c in range(chunks)]
    from_start, to_end = [], []
    run = jnp.zeros_like(totals[0])
    for c in range(chunks):
        from_start.append(early[rows[c]] * jnp.exp(run))
        run = run + totals[c]
    whole = jnp.exp(run)
    run = jnp.zeros_like(totals[0])
    for c in reversed(range(chunks)):
        to_end.append(late[rows[c]] * jnp.exp(run))
        run = run + totals[c]
    return jnp.concatenate(from_start, 0), jnp.concatenate(to_end[::-1], 0), whole


def first_head(shape):
    return lax.broadcasted_iota(jnp.int32, shape, len(shape) - 1) < (LANES // 2)


def by_head(x):
    keep = first_head(x.shape)
    zero = jnp.zeros_like(x)
    return jnp.concatenate([jnp.where(keep, x, zero), jnp.where(keep, zero, x)], 0)


def diagonal(x):
    half = x.shape[0] // 2
    return jnp.where(first_head((half, LANES)), x[:half], x[half:])


def state_kernel(pairs, fast, flag, r, k, v, f, dy, init, *outs):
    toks = r.shape[0]
    tri = triangles(toks)
    step = pl.program_id(0)
    for p in range(pairs):
        at = slice(p * LANES, (p + 1) * LANES)
        early, late, totals, _ = decays(f[:, at], tri)
        from_start, to_end, whole = spread(early, late, totals)
        key_hi, key_lo = split(k[:, at].astype(F32) * to_end)
        rec_hi, rec_lo = split(r[:, at].astype(F32) * from_start)
        state = dot(v[:, at], jnp.concatenate([key_hi, key_lo], 1), (0, 0))
        grad = dot(dy[:, at], jnp.concatenate([rec_hi, rec_lo], 1), (0, 0))
        state = diagonal(state[:, :LANES] + state[:, LANES:])
        grad = diagonal(grad[:, :LANES] + grad[:, LANES:])
        if fast:
            sent, kept, swapped = outs
            half = grad.shape[0] // 2
            is_first = flag[0] == 0
            end = whole * init[:, at] + state
            swapped[p] = jnp.where(is_first, end, grad)
            pair = step * pairs + p
            sent[pair] = jnp.where(is_first, grad[half:], grad[:half])
            kept[p] = jnp.where(is_first, grad[:half], grad[half:])
            sent[sent.shape[0] - 1, pl.ds(pair, 1), :] = whole
        else:
            states, grads, wholes = outs
            states[p] = state
            grads[p] = grad
            wholes[p] = whole


def inner_kernel(pairs, r, k, v, f, dy, boost, rec, key, val, from_out, to_out):
    toks = r.shape[0]
    chunks = toks // CHUNK
    tri = triangles(toks)
    keep = first_head((toks, LANES))
    keep_chunk = first_head((CHUNK, LANES))
    row = lax.broadcasted_iota(jnp.int32, (CHUNK, CHUNK), 0)
    col = lax.broadcasted_iota(jnp.int32, (CHUNK, CHUNK), 1)
    wide_row = lax.broadcasted_iota(jnp.int32, (toks, toks), 0)
    wide_col = lax.broadcasted_iota(jnp.int32, (toks, toks), 1)
    below = wide_col < wide_row
    reversed_tok = (chunks - 1 - wide_col // CHUNK) * CHUNK + wide_col % CHUNK
    above = reversed_tok > wide_row

    def flip(x):
        return jnp.concatenate(
            [x[c * CHUNK : (c + 1) * CHUNK] for c in reversed(range(chunks))], 0
        )

    rows = [slice(c * CHUNK, (c + 1) * CHUNK) for c in range(chunks)]
    for p in range(pairs):
        at = slice(p * LANES, (p + 1) * LANES)
        early, late, totals, middles = decays(f[:, at], tri)
        from_start, to_end, _ = spread(early, late, totals)
        from_out[:, at] = from_start
        to_out[:, at] = to_end
        rb, kb, vb, db = r[:, at], k[:, at], v[:, at], dy[:, at]
        rf, kf, vf, df = (x.astype(F32) for x in (rb, kb, vb, db))
        u = boost[:, at]
        rec_early = rf * early
        key_late = kf * late
        dy_heads = by_head(flip(db))
        scores = dot(db, by_head(vb), (1, 1))
        scores_t = dot(vb, dy_heads, (1, 1))
        scores_split, scores_t_split = [], []
        for h in range(2):
            part = slice(h * toks, (h + 1) * toks)
            scores_split.append(split(jnp.where(below, scores[:, part], 0.0)))
            scores_t_split.append(split(jnp.where(above, scores_t[:, part], 0.0)))
        rec_rows, key_rows, cross_rows = [], [], []
        for c in range(chunks):
            here = rows[c]
            count = (c + 1) * CHUNK
            pieces = [key_late[here] * jnp.exp(middles[c] - totals[c])]
            gap = middles[c]
            for e in reversed(range(c)):
                pieces.append(key_late[rows[e]] * jnp.exp(gap))
                gap = gap + totals[e]
            key_hi, key_lo = split(jnp.concatenate(pieces[::-1], 0))
            stack = jnp.concatenate(
                [s[i][here, :count] for i in range(2) for s in scores_split], 0
            )
            got = dot(stack, jnp.concatenate([key_hi, key_lo], 1))
            got = got[:, :LANES] + got[:, LANES:]
            got = got[: 2 * CHUNK] + got[2 * CHUNK :]
            got = jnp.where(keep_chunk, got[:CHUNK], got[CHUNK:])
            rec_rows.append(early[here] * jnp.exp(-middles[c]) * got)
            pieces = [rec_early[here] * jnp.exp(-middles[c])]
            gap = totals[c] - middles[c]
            for e in range(c + 1, chunks):
                pieces.append(rec_early[rows[e]] * jnp.exp(gap))
                gap = gap + totals[e]
            rec_hi, rec_lo = split(jnp.concatenate(pieces[::-1], 0))
            count = (chunks - c) * CHUNK
            stack = jnp.concatenate(
                [s[i][here, :count] for i in range(2) for s in scores_t_split], 0
            )
            got = dot(stack, jnp.concatenate([rec_hi, rec_lo], 1))
            got = got[:, :LANES] + got[:, LANES:]
            got = got[: 2 * CHUNK] + got[2 * CHUNK :]
            got = jnp.where(keep_chunk, got[:CHUNK], got[CHUNK:])
            key_rows.append(late[here] * jnp.exp(middles[c] - totals[c]) * got)
            own = slice(c * CHUNK, (c + 1) * CHUNK)
            lhs = jnp.concatenate([by_head(key_hi[own]), by_head(key_lo[own])], 0)
            if c:
                pad = jnp.zeros((c * CHUNK, LANES), BF16)
                rhs = jnp.concatenate([rec_hi, pad, rec_lo, pad], 0)
            else:
                rhs = jnp.concatenate([rec_hi, rec_lo], 0)
            got = dot(lhs, rhs, (1, 1))
            got = got[:, :toks] + got[:, toks:]
            got = got[: 2 * CHUNK] + got[2 * CHUNK :]
            cross_rows.append(
                [jnp.where(above[here], got[h * CHUNK : (h + 1) * CHUNK], 0.0) for h in range(2)]
            )
        cross = jnp.concatenate(
            [jnp.concatenate([c[h] for c in cross_rows], 0) for h in range(2)], 1
        )
        cross_hi, cross_lo = split(cross)
        inner_val = dot(cross_hi, dy_heads) + dot(cross_lo, dy_heads)
        prod = vf * df
        mix = rf * u * kf

        def head_sum(x):
            one = jnp.sum(jnp.where(keep, x, 0.0), axis=-1, keepdims=True)
            two = jnp.sum(jnp.where(keep, 0.0, x), axis=-1, keepdims=True)
            return jnp.where(keep, one, two)

        boosted = u * head_sum(prod)
        rec[:, at] = jnp.concatenate(rec_rows, 0) + kf * boosted
        key[:, at] = jnp.concatenate(key_rows, 0) + rf * boosted
        val[:, at] = inner_val + head_sum(mix) * df


def outer_kernel(
    pairs, fast, flag, k, v, dy, from_start, to_end, rec, key, val, init, state, grad, *outs
):
    rec_out, key_out, val_out = outs
    for p in range(pairs):
        at = slice(p * LANES, (p + 1) * LANES)
        if fast:
            is_first = flag[0] == 0
            got = state[p]
            start = jnp.where(is_first, init[:, at], got)
            after = jnp.where(is_first, got, 0.0)
        else:
            start = state[p]
            after = grad[p]
        start_hi, start_lo = split(by_head(start))
        after_hi, after_lo = split(by_head(after))
        db, vb = dy[:, at], v[:, at]
        from_state = dot(
            jnp.concatenate([db, db], 1), jnp.concatenate([start_hi, start_lo], 0)
        )
        rec_out[:, at] = (rec[:, at] + from_start[:, at] * from_state).astype(BF16)
        from_grad = dot(jnp.concatenate([vb, vb], 1), jnp.concatenate([after_hi, after_lo], 0))
        tail = to_end[:, at]
        key_out[:, at] = (key[:, at] + tail * from_grad).astype(BF16)
        key_hi, key_lo = split(k[:, at].astype(F32) * tail)
        wide = dot(key_hi, jnp.concatenate([after_hi, after_lo], 0), (1, 1))
        from_key = wide[:, :LANES] + wide[:, LANES:] + dot(key_lo, after_hi, (1, 1))
        val_out[:, at] = (val[:, at] + from_key).astype(BF16)


def on_device(seq_size, dp_size, r, k, v, f, boost, dy, init):
    batch, toks, width = r.shape
    heads, feature = boost.shape
    pairs = width // LANES
    group = 4 if pairs % 4 == 0 else 1
    grid = (pairs // group,)
    half = feature // 2
    block = group * LANES
    fast = (
        batch == 1
        and seq_size == 2
        and dp_size & (dp_size - 1) == 0
        and pairs % dp_size == 0
        and pairs <= half
    )
    seq = lax.axis_index("seq")
    is_first = seq == 0
    flag = jnp.reshape(seq, (1,)).astype(jnp.int32)
    boost_row = boost.reshape(1, width)
    init_t = init.T

    rows = pl.BlockSpec((toks, block), lambda i: (0, i))
    wide = pl.BlockSpec((feature, block), lambda i: (0, i))
    per_pair = pl.BlockSpec((group, feature, LANES), lambda i: (i, 0, 0))
    half_pair = pl.BlockSpec((group, half, LANES), lambda i: (i, 0, 0))
    scalar = pl.BlockSpec(memory_space=pltpu.SMEM)
    params = pltpu.CompilerParams(
        dimension_semantics=("arbitrary",), vmem_limit_bytes=24 * 2**20
    )

    def like(shape, kind=F32):
        return jax.ShapeDtypeStruct(shape, kind)

    def states(b):
        if fast:
            shapes = (
                like((pairs + 1, half, LANES)),
                like((pairs, half, LANES)),
                like((pairs, feature, LANES)),
            )
            specs = (
                pl.BlockSpec((pairs + 1, half, LANES), lambda i: (0, 0, 0)),
                half_pair,
                per_pair,
            )
        else:
            shapes = (
                like((pairs, feature, LANES)),
                like((pairs, feature, LANES)),
                like((pairs, 1, LANES)),
            )
            specs = (per_pair, per_pair, pl.BlockSpec((group, 1, LANES), lambda i: (i, 0, 0)))

        def body(*refs):
            state_kernel(group, fast, *refs)

        return pl.pallas_call(
            body,
            grid=grid,
            in_specs=[scalar] + [rows] * 5 + [wide],
            out_specs=specs,
            out_shape=shapes,
            compiler_params=params,
            name="states",
            cost_estimate=pl.CostEstimate(
                flops=4 * 10**9, bytes_accessed=4 * 2**20, transcendentals=10**6
            ),
        )(flag, r[b], k[b], v[b], f[b], dy[b], init_t)

    def inner(b):
        def body(*refs):
            inner_kernel(group, *refs)

        return pl.pallas_call(
            body,
            grid=grid,
            in_specs=[rows] * 5 + [pl.BlockSpec((1, block), lambda i: (0, i))],
            out_specs=(rows,) * 5,
            out_shape=(like((toks, width)),) * 5,
            compiler_params=params,
            name="inner",
            cost_estimate=pl.CostEstimate(
                flops=10**10, bytes_accessed=8 * 2**20, transcendentals=10**6
            ),
        )(r[b], k[b], v[b], f[b], dy[b], boost_row)

    def outer(b, partial, state, grad):
        rec, key, val, from_start, to_end = partial

        def body(*refs):
            outer_kernel(group, fast, *refs)

        return pl.pallas_call(
            body,
            grid=grid,
            in_specs=[scalar] + [rows] * 8 + [wide, per_pair, per_pair],
            out_specs=(rows,) * 3,
            out_shape=(like((toks, width), BF16),) * 3,
            compiler_params=params,
            name="outer",
            cost_estimate=pl.CostEstimate(
                flops=3 * 10**9, bytes_accessed=9 * 2**20, transcendentals=0
            ),
        )(flag, k[b], v[b], dy[b], from_start, to_end, rec, key, val, init_t, state, grad)

    if fast:
        sent, kept, swapped = states(0)
        swap = [(0, 1), (1, 0)]
        got = lax.ppermute(sent, "seq", swap)
        other = lax.ppermute(swapped, "seq", swap)
        partial = inner(0)
        whole = jnp.where(is_first, sent[pairs, :pairs], got[pairs, :pairs])[:, None, :]
        total = jnp.where(is_first, kept, got[:pairs]) + whole * jnp.where(
            is_first, got[:pairs], kept
        )
        place = lax.axis_index("dp")
        total = total.reshape(dp_size, pairs // dp_size, half, LANES)
        bit = 1
        while bit < dp_size:
            couples = total.reshape((total.shape[0] // 2, 2) + total.shape[1:])
            upper = (place & bit) != 0
            mine = jnp.where(upper, couples[:, 1], couples[:, 0])
            theirs = jnp.where(upper, couples[:, 0], couples[:, 1])
            total = mine + lax.ppermute(
                theirs, "dp", [(i, i ^ bit) for i in range(dp_size)]
            )
            bit *= 2
        state_grad = total[0].transpose(0, 2, 1).reshape(-1, half)
        rec, key, val = outer(0, partial, other, other)
        return rec[None], key[None], val[None], state_grad

    forward = [(i, i + 1) for i in range(seq_size - 1)]
    backward = [(i + 1, i) for i in range(seq_size - 1)]
    start_t = init_t.reshape(feature, pairs, LANES).transpose(1, 0, 2)
    results, term = [], 0.0
    for b in range(batch):
        state_local, grad_local, whole = states(b)
        start = start_t
        after = jnp.zeros_like(grad_local)
        for _ in range(seq_size - 1):
            end = whole * start + state_local
            start = jnp.where(is_first, start_t, lax.ppermute(end, "seq", forward))
            after = lax.ppermute(grad_local + whole * after, "seq", backward)
        results.append(outer(b, inner(b), start, after))
        term = term + jnp.where(is_first, grad_local + whole * after, 0.0)
    term = term.transpose(0, 2, 1).reshape(width, feature)
    summed = lax.psum_scatter(term, "dp", scatter_dimension=0, tiled=True)
    summed = lax.psum(summed, "seq")
    columns = feature // seq_size
    state_grad = lax.dynamic_slice_in_dim(summed, seq * columns, columns, 1)
    rec, key, val = (jnp.stack(x) for x in zip(*results))
    return rec, key, val, state_grad


def solution(mesh):
    sizes = dict(mesh.shape)
    rows = P("dp", "seq", None)

    def run(*args):
        return on_device(sizes["seq"], sizes["dp"], *args)

    return jax.shard_map(
        run,
        mesh=mesh,
        in_specs=(rows, rows, rows, rows, P(), rows, P()),
        out_specs=(rows, rows, rows, P("dp", "seq")),
        check_vma=False,
    )
```

```python
import jax
import jax.numpy as jnp
from jax import lax
from jax.experimental import pallas as pl
from jax.experimental.pallas import tpu as pltpu
from jax.sharding import PartitionSpec as P


LANES = 128
CHUNK = 32
UNROLL = 4
BF16 = jnp.bfloat16
F32 = jnp.float32


def dot(a, b, contract=(1, 0)):
    return lax.dot_general(
        a, b, (((contract[0],), (contract[1],)), ((), ())), preferred_element_type=F32
    )


def split(x):
    hi = x.astype(BF16)
    return hi, (x - hi.astype(F32)).astype(BF16)


def triangles(toks):
    row = lax.broadcasted_iota(jnp.int32, (toks, toks), 0)
    col = lax.broadcasted_iota(jnp.int32, (toks, toks), 1)
    same = (row // CHUNK) == (col // CHUNK)
    before = jnp.where(same & (col < row), 1.0, 0.0).astype(BF16)
    after = jnp.where(same & (col > row), 1.0, 0.0).astype(BF16)
    return jnp.concatenate([before, after], 0)


def decays(fade, tri):
    toks = fade.shape[0]
    log_decay = -jnp.exp(fade.astype(F32))
    hi, lo = split(log_decay)
    sums = dot(jnp.concatenate([tri, tri], 1), jnp.concatenate([hi, lo], 0))
    prefix, suffix = sums[:toks], sums[toks:]
    totals, middles = [], []
    for c in range(toks // CHUNK):
        last = (c + 1) * CHUNK - 1
        totals.append(prefix[last : last + 1] + log_decay[last : last + 1])
        mid = c * CHUNK + CHUNK // 2
        middles.append(prefix[mid : mid + 1])
    return jnp.exp(prefix), jnp.exp(suffix), totals, middles


def spread(early, late, totals):
    chunks = len(totals)
    rows = [slice(c * CHUNK, (c + 1) * CHUNK) for c in range(chunks)]
    from_start, to_end = [], []
    run = jnp.zeros_like(totals[0])
    for c in range(chunks):
        from_start.append(early[rows[c]] * jnp.exp(run))
        run = run + totals[c]
    whole = jnp.exp(run)
    run = jnp.zeros_like(totals[0])
    for c in reversed(range(chunks)):
        to_end.append(late[rows[c]] * jnp.exp(run))
        run = run + totals[c]
    return jnp.concatenate(from_start, 0), jnp.concatenate(to_end[::-1], 0), whole


def first_head(shape):
    return lax.broadcasted_iota(jnp.int32, shape, len(shape) - 1) < (LANES // 2)


def by_head(x):
    keep = first_head(x.shape)
    zero = jnp.zeros_like(x)
    return jnp.concatenate([jnp.where(keep, x, zero), jnp.where(keep, zero, x)], 0)


def diagonal(x):
    half = x.shape[0] // 2
    return jnp.where(first_head((half, LANES)), x[:half], x[half:])


def state_kernel(group, fast, *refs):
    sources, refs = refs[:6], refs[6:]
    copies, refs = refs[:6], refs[6:]
    outs, sems = refs[:-1], refs[-1]
    r, k, v, f, dy, init = copies
    toks, width = r.shape
    steps = width // LANES // group
    is_first = lax.axis_index("seq") == 0

    def fetch(step, i):
        lanes = pl.ds(step * group * LANES, group * LANES)
        return pltpu.make_async_copy(
            sources[i].at[:, lanes], copies[i].at[:, lanes], sems.at[step, i]
        )

    order = (3, 0, 4, 1, 2, 5)
    for step in range(steps):
        for i in order:
            fetch(step, i).start()
    tri = triangles(toks)
    for step in range(steps):
        for i in order:
            fetch(step, i).wait()
        for pair in range(step * group, (step + 1) * group):
            at = slice(pair * LANES, (pair + 1) * LANES)
            early, late, totals, _ = decays(f[:, at], tri)
            from_start, to_end, whole = spread(early, late, totals)
            key_hi, key_lo = split(k[:, at].astype(F32) * to_end)
            rec_hi, rec_lo = split(r[:, at].astype(F32) * from_start)
            state = dot(v[:, at], jnp.concatenate([key_hi, key_lo], 1), (0, 0))
            grad = dot(dy[:, at], jnp.concatenate([rec_hi, rec_lo], 1), (0, 0))
            state = diagonal(state[:, :LANES] + state[:, LANES:])
            grad = diagonal(grad[:, :LANES] + grad[:, LANES:])
            if fast:
                sent, kept, swapped = outs
                half = grad.shape[0] // 2
                end = whole * init[:, at] + state
                swapped[pair] = jnp.where(is_first, end, grad)
                sent[pair] = jnp.where(is_first, grad[half:], grad[:half])
                kept[pair] = jnp.where(is_first, grad[:half], grad[half:])
                sent[sent.shape[0] - 1, pair : pair + 1] = whole
            else:
                states, grads, wholes = outs
                states[pair] = state
                grads[pair] = grad
                wholes[pair] = whole


def inner_kernel(first, count, unroll, r, k, v, f, dy, boost, *outs):
    def step(i, carry):
        base = pl.multiple_of(i * unroll * LANES, LANES)
        inner_pairs(first * LANES + base, base, unroll, r, k, v, f, dy, boost, *outs)
        return carry

    lax.fori_loop(0, count // unroll, step, 0)


def inner_pairs(base, out_base, pairs, r, k, v, f, dy, boost, rec, key, val, from_out, to_out):
    toks = r.shape[0]
    chunks = toks // CHUNK
    tri = triangles(toks)
    keep = first_head((toks, LANES))
    keep_chunk = first_head((CHUNK, LANES))
    row = lax.broadcasted_iota(jnp.int32, (CHUNK, CHUNK), 0)
    col = lax.broadcasted_iota(jnp.int32, (CHUNK, CHUNK), 1)
    wide_row = lax.broadcasted_iota(jnp.int32, (toks, toks), 0)
    wide_col = lax.broadcasted_iota(jnp.int32, (toks, toks), 1)
    below = wide_col < wide_row
    reversed_tok = (chunks - 1 - wide_col // CHUNK) * CHUNK + wide_col % CHUNK
    above = reversed_tok > wide_row

    def flip(x):
        return jnp.concatenate(
            [x[c * CHUNK : (c + 1) * CHUNK] for c in reversed(range(chunks))], 0
        )

    rows = [slice(c * CHUNK, (c + 1) * CHUNK) for c in range(chunks)]
    for p in range(pairs):
        at = pl.ds(pl.multiple_of(base + p * LANES, LANES), LANES)
        to = pl.ds(pl.multiple_of(out_base + p * LANES, LANES), LANES)
        early, late, totals, middles = decays(f[:, at], tri)
        from_start, to_end, _ = spread(early, late, totals)
        from_out[:, to] = from_start
        to_out[:, to] = to_end
        rb, kb, vb, db = r[:, at], k[:, at], v[:, at], dy[:, at]
        rf, kf, vf, df = (x.astype(F32) for x in (rb, kb, vb, db))
        head = 2 * (base // LANES + p)
        u = jnp.concatenate([boost[pl.ds(head, 1)], boost[pl.ds(head + 1, 1)]], 1)
        rec_early = rf * early
        key_late = kf * late
        dy_heads = by_head(flip(db))
        scores = dot(db, by_head(vb), (1, 1))
        scores_t = dot(vb, dy_heads, (1, 1))
        scores_split, scores_t_split = [], []
        for h in range(2):
            part = slice(h * toks, (h + 1) * toks)
            scores_split.append(split(jnp.where(below, scores[:, part], 0.0)))
            scores_t_split.append(split(jnp.where(above, scores_t[:, part], 0.0)))
        rec_rows, key_rows, cross_rows = [], [], []
        for c in range(chunks):
            here = rows[c]
            count = (c + 1) * CHUNK
            pieces = [key_late[here] * jnp.exp(middles[c] - totals[c])]
            gap = middles[c]
            for e in reversed(range(c)):
                pieces.append(key_late[rows[e]] * jnp.exp(gap))
                gap = gap + totals[e]
            key_hi, key_lo = split(jnp.concatenate(pieces[::-1], 0))
            stack = jnp.concatenate(
                [s[i][here, :count] for i in range(2) for s in scores_split], 0
            )
            got = dot(stack, jnp.concatenate([key_hi, key_lo], 1))
            got = got[:, :LANES] + got[:, LANES:]
            got = got[: 2 * CHUNK] + got[2 * CHUNK :]
            got = jnp.where(keep_chunk, got[:CHUNK], got[CHUNK:])
            rec_rows.append(early[here] * jnp.exp(-middles[c]) * got)
            pieces = [rec_early[here] * jnp.exp(-middles[c])]
            gap = totals[c] - middles[c]
            for e in range(c + 1, chunks):
                pieces.append(rec_early[rows[e]] * jnp.exp(gap))
                gap = gap + totals[e]
            rec_hi, rec_lo = split(jnp.concatenate(pieces[::-1], 0))
            count = (chunks - c) * CHUNK
            stack = jnp.concatenate(
                [s[i][here, :count] for i in range(2) for s in scores_t_split], 0
            )
            got = dot(stack, jnp.concatenate([rec_hi, rec_lo], 1))
            got = got[:, :LANES] + got[:, LANES:]
            got = got[: 2 * CHUNK] + got[2 * CHUNK :]
            got = jnp.where(keep_chunk, got[:CHUNK], got[CHUNK:])
            key_rows.append(late[here] * jnp.exp(middles[c] - totals[c]) * got)
            own = slice(c * CHUNK, (c + 1) * CHUNK)
            lhs = jnp.concatenate([by_head(key_hi[own]), by_head(key_lo[own])], 0)
            if c:
                pad = jnp.zeros((c * CHUNK, LANES), BF16)
                rhs = jnp.concatenate([rec_hi, pad, rec_lo, pad], 0)
            else:
                rhs = jnp.concatenate([rec_hi, rec_lo], 0)
            got = dot(lhs, rhs, (1, 1))
            got = got[:, :toks] + got[:, toks:]
            got = got[: 2 * CHUNK] + got[2 * CHUNK :]
            cross_rows.append(
                [jnp.where(above[here], got[h * CHUNK : (h + 1) * CHUNK], 0.0) for h in range(2)]
            )
        cross = jnp.concatenate(
            [jnp.concatenate([c[h] for c in cross_rows], 0) for h in range(2)], 1
        )
        cross_hi, cross_lo = split(cross)
        inner_val = dot(cross_hi, dy_heads) + dot(cross_lo, dy_heads)
        prod = vf * df
        mix = rf * u * kf

        def head_sum(x):
            one = jnp.sum(jnp.where(keep, x, 0.0), axis=-1, keepdims=True)
            two = jnp.sum(jnp.where(keep, 0.0, x), axis=-1, keepdims=True)
            return jnp.where(keep, one, two)

        boosted = u * head_sum(prod)
        rec[:, to] = jnp.concatenate(rec_rows, 0) + kf * boosted
        key[:, to] = jnp.concatenate(key_rows, 0) + rf * boosted
        val[:, to] = inner_val + head_sum(mix) * df


def outer_kernel(
    first, pairs, fast, k, v, dy, from_start, to_end, rec, key, val, init, *refs
):
    state, grad = refs[0], refs[-4]
    rec_out, key_out, val_out = refs[-3:]
    is_first = lax.axis_index("seq") == 0
    step = pl.program_id(0)
    for p in range(pairs):
        here = step * pairs + p
        at = pl.ds(pl.multiple_of((first + here) * LANES, LANES), LANES)
        part = pl.ds(pl.multiple_of(here * LANES, LANES), LANES)
        out = slice(p * LANES, (p + 1) * LANES)
        if fast:
            got = state[first + here]
            start = jnp.where(is_first, init[:, at], got)
            after = jnp.where(is_first, got, 0.0)
        else:
            start = state[first + here]
            after = grad[first + here]
        start_hi, start_lo = split(by_head(start))
        after_hi, after_lo = split(by_head(after))
        db, vb = dy[:, at], v[:, at]
        from_state = dot(
            jnp.concatenate([db, db], 1), jnp.concatenate([start_hi, start_lo], 0)
        )
        rec_out[:, out] = (rec[:, part] + from_start[:, part] * from_state).astype(BF16)
        from_grad = dot(jnp.concatenate([vb, vb], 1), jnp.concatenate([after_hi, after_lo], 0))
        tail = to_end[:, part]
        key_out[:, out] = (key[:, part] + tail * from_grad).astype(BF16)
        key_hi, key_lo = split(k[:, at].astype(F32) * tail)
        wide = dot(key_hi, jnp.concatenate([after_hi, after_lo], 0), (1, 1))
        from_key = wide[:, :LANES] + wide[:, LANES:] + dot(key_lo, after_hi, (1, 1))
        val_out[:, out] = (val[:, part] + from_key).astype(BF16)


def share_kernel(blocks, sent, kept, got, mine, theirs):
    is_first = lax.axis_index("seq") == 0
    upper = lax.axis_index("dp") & 1
    last = sent.shape[0] - 1
    for b in range(blocks // 2):
        for ref, low in ((mine, upper), (theirs, 1 - upper)):
            p = 2 * b + low
            whole = jnp.where(is_first, sent[last, pl.ds(p, 1), :], got[last, pl.ds(p, 1), :])
            own, other = kept[p], got[p]
            ref[b] = jnp.where(is_first, own, other) + whole * jnp.where(is_first, other, own)


def halve_kernel(bit, mine, got, kept, theirs):
    upper = (lax.axis_index("dp") // bit) & 1
    for b in range(kept.shape[0]):
        for ref, low in ((kept, upper), (theirs, 1 - upper)):
            ref[b] = mine[2 * b + low] + got[2 * b + low]


def on_device(seq_size, dp_size, r, k, v, f, boost, dy, init):
    batch, toks, width = r.shape
    _, feature = boost.shape
    pairs = width // LANES
    group = 4 if pairs % 4 == 0 else 1
    half = feature // 2
    fast = (
        batch == 1
        and seq_size == 2
        and dp_size & (dp_size - 1) == 0
        and pairs == dp_size
        and pairs <= half
    )
    seq = lax.axis_index("seq")
    is_first = seq == 0
    init_t = init.T

    vmem = pl.BlockSpec(memory_space=pltpu.VMEM)
    anywhere = pl.BlockSpec(memory_space=pl.ANY)

    def limit(mib):
        return pltpu.CompilerParams(vmem_limit_bytes=mib * 2**20)

    def like(shape, kind=F32):
        return jax.ShapeDtypeStruct(shape, kind)

    def in_hbm(x):
        return pltpu.with_memory_space_constraint(x, pltpu.HBM)

    def states(b):
        if fast:
            shapes = (
                like((pairs + 1, half, LANES)),
                like((pairs, half, LANES)),
                like((pairs, feature, LANES)),
            )
        else:
            shapes = (
                like((pairs, feature, LANES)),
                like((pairs, feature, LANES)),
                like((pairs, 1, LANES)),
            )
        operands = (r[b], k[b], v[b], f[b], dy[b], init_t)
        outs = pl.pallas_call(
            lambda *refs: state_kernel(group, fast, *refs),
            in_specs=[anywhere] * 6,
            out_specs=(vmem,) * 9,
            out_shape=tuple(like(x.shape, x.dtype) for x in operands) + shapes,
            scratch_shapes=[pltpu.SemaphoreType.DMA((pairs // group, 6))],
            compiler_params=limit(24),
            name="states",
            cost_estimate=pl.CostEstimate(
                flops=4 * 10**9, bytes_accessed=4 * 2**20, transcendentals=10**6
            ),
        )(*(in_hbm(x) for x in operands))
        return outs[:6], outs[6:]

    def inner(near, first=0, count=pairs):
        def body(*refs):
            inner_kernel(first, count, UNROLL if count % UNROLL == 0 else 1, *refs)

        return pl.pallas_call(
            body,
            in_specs=[vmem] * 6,
            out_specs=(vmem,) * 5,
            out_shape=(like((toks, count * LANES)),) * 5,
            compiler_params=limit(24),
            name="inner",
            cost_estimate=pl.CostEstimate(
                flops=10**10, bytes_accessed=8 * 2**20, transcendentals=10**6
            ),
        )(*near[:5], boost)

    def outer(near, partial, carried, first=0, count=pairs, prior=()):
        rec, key, val, from_start, to_end = partial
        _, k, v, _, dy, start = near
        group = 4 if count % 4 == 0 else 1
        block = group * LANES

        def body(*refs):
            given = 9 + len(carried)
            outer_kernel(first, group, fast, *refs[:given], *refs[given + len(prior) :])

        here = pl.BlockSpec((toks, block), lambda i: (0, i + first // group))
        return pl.pallas_call(
            body,
            grid=(count // group,),
            in_specs=[vmem] * (9 + len(carried)) + [anywhere] * len(prior),
            out_specs=(here,) * 3,
            out_shape=(like((toks, width), BF16),) * 3,
            input_output_aliases={9 + len(carried) + i: i for i in range(len(prior))},
            compiler_params=limit(24),
            name="outer",
            cost_estimate=pl.CostEstimate(
                flops=3 * 10**9, bytes_accessed=9 * 2**20, transcendentals=0
            ),
        )(k, v, dy, from_start, to_end, rec, key, val, start, *carried, *prior)

    def share(sent, kept, got):
        shape = like((pairs // 2, half, LANES))
        return pl.pallas_call(
            lambda *refs: share_kernel(pairs, *refs),
            in_specs=[vmem] * 3,
            out_specs=(vmem,) * 2,
            out_shape=(shape,) * 2,
            compiler_params=limit(2),
            name="share",
        )(sent, kept, got)

    def halve(bit, mine, got):
        shape = like((mine.shape[0] // 2,) + mine.shape[1:])
        return pl.pallas_call(
            lambda *refs: halve_kernel(bit, *refs),
            in_specs=[vmem] * 2,
            out_specs=(vmem,) * 2,
            out_shape=(shape,) * 2,
            compiler_params=limit(2),
            name="halve",
        )(mine, got)

    if fast:
        near, (sent, kept, swapped) = states(0)
        swap = [(0, 1), (1, 0)]
        got = lax.ppermute(sent, "seq", swap)
        other = lax.ppermute(swapped, "seq", swap)
        cut = 3 * pairs // 4
        partial_a = inner(near, 0, cut)
        partial_b = inner(near, cut, pairs - cut)
        mine, theirs = share(sent, kept, got)
        bit = 1
        while True:
            got = lax.ppermute(theirs, "dp", [(i, i ^ bit) for i in range(dp_size)])
            bit *= 2
            if bit == dp_size:
                break
            mine, theirs = halve(bit, mine, got)
        total = mine + got
        state_grad = total.transpose(0, 2, 1).reshape(-1, half)
        results = outer(near, partial_a, (other,), 0, cut)
        rec, key, val = outer(near, partial_b, (other,), cut, pairs - cut, results)
        return rec[None], key[None], val[None], state_grad

    forward = [(i, i + 1) for i in range(seq_size - 1)]
    backward = [(i + 1, i) for i in range(seq_size - 1)]
    start_t = init_t.reshape(feature, pairs, LANES).transpose(1, 0, 2)
    results, term = [], 0.0
    for b in range(batch):
        near, (state_local, grad_local, whole) = states(b)
        start = start_t
        after = jnp.zeros_like(grad_local)
        for _ in range(seq_size - 1):
            end = whole * start + state_local
            start = jnp.where(is_first, start_t, lax.ppermute(end, "seq", forward))
            after = lax.ppermute(grad_local + whole * after, "seq", backward)
        results.append(outer(near, inner(near), (start, after)))
        term = term + jnp.where(is_first, grad_local + whole * after, 0.0)
    term = term.transpose(0, 2, 1).reshape(width, feature)
    summed = lax.psum_scatter(term, "dp", scatter_dimension=0, tiled=True)
    summed = lax.psum(summed, "seq")
    columns = feature // seq_size
    state_grad = lax.dynamic_slice_in_dim(summed, seq * columns, columns, 1)
    rec, key, val = (jnp.stack(x) for x in zip(*results))
    return rec, key, val, state_grad


def solution(mesh):
    sizes = dict(mesh.shape)
    rows = P("dp", "seq", None)

    def run(*args):
        return on_device(sizes["seq"], sizes["dp"], *args)

    return jax.shard_map(
        run,
        mesh=mesh,
        in_specs=(rows, rows, rows, rows, P(), rows, P()),
        out_specs=(rows, rows, rows, P("dp", "seq")),
        check_vma=False,
    )
```

```python
import jax
import jax.numpy as jnp
from jax import lax
from jax.experimental import pallas as pl
from jax.experimental.pallas import tpu as pltpu
from jax.sharding import PartitionSpec as P


LANES = 128
CHUNK = 32
UNROLL = 4
BF16 = jnp.bfloat16
F32 = jnp.float32


def dot(a, b, contract=(1, 0)):
    return lax.dot_general(
        a, b, (((contract[0],), (contract[1],)), ((), ())), preferred_element_type=F32
    )


def split(x):
    hi = x.astype(BF16)
    return hi, (x - hi.astype(F32)).astype(BF16)


def triangles(toks):
    row = lax.broadcasted_iota(jnp.int32, (toks, toks), 0)
    col = lax.broadcasted_iota(jnp.int32, (toks, toks), 1)
    same = (row // CHUNK) == (col // CHUNK)
    before = jnp.where(same & (col < row), 1.0, 0.0).astype(BF16)
    after = jnp.where(same & (col > row), 1.0, 0.0).astype(BF16)
    return jnp.concatenate([before, after], 0)


def decays(fade, tri):
    toks = fade.shape[0]
    log_decay = -jnp.exp(fade.astype(F32))
    hi, lo = split(log_decay)
    sums = dot(jnp.concatenate([tri, tri], 1), jnp.concatenate([hi, lo], 0))
    prefix, suffix = sums[:toks], sums[toks:]
    totals, middles = [], []
    for c in range(toks // CHUNK):
        last = (c + 1) * CHUNK - 1
        totals.append(prefix[last : last + 1] + log_decay[last : last + 1])
        mid = c * CHUNK + CHUNK // 2
        middles.append(prefix[mid : mid + 1])
    return jnp.exp(prefix), jnp.exp(suffix), totals, middles


def spread(early, late, totals):
    chunks = len(totals)
    rows = [slice(c * CHUNK, (c + 1) * CHUNK) for c in range(chunks)]
    from_start, to_end = [], []
    run = jnp.zeros_like(totals[0])
    for c in range(chunks):
        from_start.append(early[rows[c]] * jnp.exp(run))
        run = run + totals[c]
    whole = jnp.exp(run)
    run = jnp.zeros_like(totals[0])
    for c in reversed(range(chunks)):
        to_end.append(late[rows[c]] * jnp.exp(run))
        run = run + totals[c]
    return jnp.concatenate(from_start, 0), jnp.concatenate(to_end[::-1], 0), whole


def first_head(shape):
    return lax.broadcasted_iota(jnp.int32, shape, len(shape) - 1) < (LANES // 2)


def by_head(x):
    keep = first_head(x.shape)
    zero = jnp.zeros_like(x)
    return jnp.concatenate([jnp.where(keep, x, zero), jnp.where(keep, zero, x)], 0)


def diagonal(x):
    half = x.shape[0] // 2
    return jnp.where(first_head((half, LANES)), x[:half], x[half:])


def state_kernel(group, fast, *refs):
    sources, refs = refs[:6], refs[6:]
    copies, refs = refs[:6], refs[6:]
    outs, sems = refs[:-1], refs[-1]
    r, k, v, f, dy, init = copies
    toks, width = r.shape
    steps = width // LANES // group
    is_first = lax.axis_index("seq") == 0

    def fetch(step, i):
        lanes = pl.ds(step * group * LANES, group * LANES)
        return pltpu.make_async_copy(
            sources[i].at[:, lanes], copies[i].at[:, lanes], sems.at[step, i]
        )

    order = (3, 0, 4, 1, 2, 5)
    for step in range(steps):
        for i in order:
            fetch(step, i).start()
    tri = triangles(toks)
    for step in range(steps):
        for i in order:
            fetch(step, i).wait()
        for pair in range(step * group, (step + 1) * group):
            at = slice(pair * LANES, (pair + 1) * LANES)
            early, late, totals, _ = decays(f[:, at], tri)
            from_start, to_end, whole = spread(early, late, totals)
            key_hi, key_lo = split(k[:, at].astype(F32) * to_end)
            rec_hi, rec_lo = split(r[:, at].astype(F32) * from_start)
            state = dot(v[:, at], jnp.concatenate([key_hi, key_lo], 1), (0, 0))
            grad = dot(dy[:, at], jnp.concatenate([rec_hi, rec_lo], 1), (0, 0))
            state = diagonal(state[:, :LANES] + state[:, LANES:])
            grad = diagonal(grad[:, :LANES] + grad[:, LANES:])
            if fast:
                sent, kept, swapped = outs
                half = grad.shape[0] // 2
                end = whole * init[:, at] + state
                swapped[pair] = jnp.where(is_first, end, grad)
                sent[pair] = jnp.where(is_first, grad[half:], grad[:half])
                kept[pair] = jnp.where(is_first, grad[:half], grad[half:])
                sent[sent.shape[0] - 1, pair : pair + 1] = whole
            else:
                states, grads, wholes = outs
                states[pair] = state
                grads[pair] = grad
                wholes[pair] = whole


def inner_kernel(first, count, unroll, r, k, v, f, dy, boost, *outs):
    def step(i, carry):
        base = pl.multiple_of(i * unroll * LANES, LANES)
        inner_pairs(first * LANES + base, base, unroll, r, k, v, f, dy, boost, *outs)
        return carry

    lax.fori_loop(0, count // unroll, step, 0)


def inner_pairs(base, out_base, pairs, r, k, v, f, dy, boost, rec, key, val, from_out, to_out):
    toks = r.shape[0]
    chunks = toks // CHUNK
    tri = triangles(toks)
    keep = first_head((toks, LANES))
    keep_chunk = first_head((CHUNK, LANES))
    row = lax.broadcasted_iota(jnp.int32, (CHUNK, CHUNK), 0)
    col = lax.broadcasted_iota(jnp.int32, (CHUNK, CHUNK), 1)
    wide_row = lax.broadcasted_iota(jnp.int32, (toks, toks), 0)
    wide_col = lax.broadcasted_iota(jnp.int32, (toks, toks), 1)
    below = wide_col < wide_row
    reversed_tok = (chunks - 1 - wide_col // CHUNK) * CHUNK + wide_col % CHUNK
    above = reversed_tok > wide_row

    def flip(x):
        return jnp.concatenate(
            [x[c * CHUNK : (c + 1) * CHUNK] for c in reversed(range(chunks))], 0
        )

    rows = [slice(c * CHUNK, (c + 1) * CHUNK) for c in range(chunks)]
    for p in range(pairs):
        at = pl.ds(pl.multiple_of(base + p * LANES, LANES), LANES)
        to = pl.ds(pl.multiple_of(out_base + p * LANES, LANES), LANES)
        early, late, totals, middles = decays(f[:, at], tri)
        from_start, to_end, _ = spread(early, late, totals)
        from_out[:, to] = from_start
        to_out[:, to] = to_end
        rb, kb, vb, db = r[:, at], k[:, at], v[:, at], dy[:, at]
        rf, kf, vf, df = (x.astype(F32) for x in (rb, kb, vb, db))
        head = 2 * (base // LANES + p)
        u = jnp.concatenate([boost[pl.ds(head, 1)], boost[pl.ds(head + 1, 1)]], 1)
        rec_early = rf * early
        key_late = kf * late
        dy_heads = by_head(flip(db))
        scores = dot(db, by_head(vb), (1, 1))
        scores_t = dot(vb, dy_heads, (1, 1))
        scores_split, scores_t_split = [], []
        for h in range(2):
            part = slice(h * toks, (h + 1) * toks)
            scores_split.append(split(jnp.where(below, scores[:, part], 0.0)))
            scores_t_split.append(split(jnp.where(above, scores_t[:, part], 0.0)))
        rec_rows, key_rows, cross_rows = [], [], []
        for c in range(chunks):
            here = rows[c]
            count = (c + 1) * CHUNK
            pieces = [key_late[here] * jnp.exp(middles[c] - totals[c])]
            gap = middles[c]
            for e in reversed(range(c)):
                pieces.append(key_late[rows[e]] * jnp.exp(gap))
                gap = gap + totals[e]
            key_hi, key_lo = split(jnp.concatenate(pieces[::-1], 0))
            stack = jnp.concatenate(
                [s[i][here, :count] for i in range(2) for s in scores_split], 0
            )
            got = dot(stack, jnp.concatenate([key_hi, key_lo], 1))
            got = got[:, :LANES] + got[:, LANES:]
            got = got[: 2 * CHUNK] + got[2 * CHUNK :]
            got = jnp.where(keep_chunk, got[:CHUNK], got[CHUNK:])
            rec_rows.append(early[here] * jnp.exp(-middles[c]) * got)
            pieces = [rec_early[here] * jnp.exp(-middles[c])]
            gap = totals[c] - middles[c]
            for e in range(c + 1, chunks):
                pieces.append(rec_early[rows[e]] * jnp.exp(gap))
                gap = gap + totals[e]
            rec_hi, rec_lo = split(jnp.concatenate(pieces[::-1], 0))
            count = (chunks - c) * CHUNK
            stack = jnp.concatenate(
                [s[i][here, :count] for i in range(2) for s in scores_t_split], 0
            )
            got = dot(stack, jnp.concatenate([rec_hi, rec_lo], 1))
            got = got[:, :LANES] + got[:, LANES:]
            got = got[: 2 * CHUNK] + got[2 * CHUNK :]
            got = jnp.where(keep_chunk, got[:CHUNK], got[CHUNK:])
            key_rows.append(late[here] * jnp.exp(middles[c] - totals[c]) * got)
            own = slice(c * CHUNK, (c + 1) * CHUNK)
            lhs = jnp.concatenate([by_head(key_hi[own]), by_head(key_lo[own])], 0)
            if c:
                pad = jnp.zeros((c * CHUNK, LANES), BF16)
                rhs = jnp.concatenate([rec_hi, pad, rec_lo, pad], 0)
            else:
                rhs = jnp.concatenate([rec_hi, rec_lo], 0)
            got = dot(lhs, rhs, (1, 1))
            got = got[:, :toks] + got[:, toks:]
            got = got[: 2 * CHUNK] + got[2 * CHUNK :]
            cross_rows.append(
                [jnp.where(above[here], got[h * CHUNK : (h + 1) * CHUNK], 0.0) for h in range(2)]
            )
        cross = jnp.concatenate(
            [jnp.concatenate([c[h] for c in cross_rows], 0) for h in range(2)], 1
        )
        cross_hi, cross_lo = split(cross)
        inner_val = dot(cross_hi, dy_heads) + dot(cross_lo, dy_heads)
        prod = vf * df
        mix = rf * u * kf

        def head_sum(x):
            one = jnp.sum(jnp.where(keep, x, 0.0), axis=-1, keepdims=True)
            two = jnp.sum(jnp.where(keep, 0.0, x), axis=-1, keepdims=True)
            return jnp.where(keep, one, two)

        boosted = u * head_sum(prod)
        rec[:, to] = jnp.concatenate(rec_rows, 0) + kf * boosted
        key[:, to] = jnp.concatenate(key_rows, 0) + rf * boosted
        val[:, to] = inner_val + head_sum(mix) * df


def state_part(rows, state):
    hi, lo = split(by_head(state))
    return dot(jnp.concatenate([rows, rows], 1), jnp.concatenate([hi, lo], 0))


def key_part(keys, state):
    hi, lo = split(by_head(state))
    key_hi, key_lo = split(keys)
    wide = dot(key_hi, jnp.concatenate([hi, lo], 0), (1, 1))
    return wide[:, :LANES] + wide[:, LANES:] + dot(key_lo, hi, (1, 1))


def outer_kernel(pairs, k, v, dy, from_start, to_end, rec, key, val, start, after, *outs):
    rec_out, key_out, val_out = outs
    for p in range(pairs):
        at = slice(p * LANES, (p + 1) * LANES)
        tail = to_end[:, at]
        from_state = state_part(dy[:, at], start[p])
        rec_out[:, at] = (rec[:, at] + from_start[:, at] * from_state).astype(BF16)
        from_grad = state_part(v[:, at], after[p])
        key_out[:, at] = (key[:, at] + tail * from_grad).astype(BF16)
        from_key = key_part(k[:, at].astype(F32) * tail, after[p])
        val_out[:, at] = (val[:, at] + from_key).astype(BF16)


class Writer:
    def __init__(self, group, held, outs, sems):
        self.group, self.held, self.outs, self.sems = group, held, outs, sems
        self.started = []

    def put(self, pair, *values):
        at = slice(pair * LANES, (pair + 1) * LANES)
        for i, value in enumerate(values):
            self.held[i, :, at] = value.astype(BF16)
        if (pair + 1) % self.group == 0:
            step = pair // self.group
            lanes = pl.ds(step * self.group * LANES, self.group * LANES)
            for i in range(len(values)):
                copy = pltpu.make_async_copy(
                    self.held.at[i, :, lanes], self.outs[i].at[:, lanes], self.sems.at[step, i]
                )
                copy.start()
                self.started.append(copy)

    def finish(self):
        for copy in self.started:
            copy.wait()


def partial_of(pair, early, late):
    count = early[0].shape[1] // LANES
    refs, place = (early, pair) if pair < count else (late, pair - count)
    return refs, slice(place * LANES, (place + 1) * LANES)


def known_kernel(group, dy, init, *refs):
    early, late, (rec_out, key_out, val_out, held, sems) = refs[:5], refs[5:10], refs[10:]
    pairs = dy.shape[1] // LANES
    is_first = lax.axis_index("seq") == 0

    @pl.when(is_first)
    def _():
        writer = Writer(group, held, (rec_out,), sems)
        for pair in range(pairs):
            (rec, _, _, from_start, _), part = partial_of(pair, early, late)
            at = slice(pair * LANES, (pair + 1) * LANES)
            from_state = state_part(dy[:, at], init[:, at])
            writer.put(pair, rec[:, part] + from_start[:, part] * from_state)
        writer.finish()

    @pl.when(jnp.logical_not(is_first))
    def _():
        writer = Writer(group, held, (key_out, val_out), sems)
        for pair in range(pairs):
            (_, key, val, _, _), part = partial_of(pair, early, late)
            writer.put(pair, key[:, part], val[:, part])
        writer.finish()


def swapped_kernel(group, k, v, dy, swapped, *refs):
    early, late, outs = refs[:5], refs[5:10], refs[-5:]
    rec_out, key_out, val_out, held, sems = outs
    pairs = dy.shape[1] // LANES
    is_first = lax.axis_index("seq") == 0

    @pl.when(is_first)
    def _():
        writer = Writer(group, held, (key_out, val_out), sems)
        for pair in range(pairs):
            (_, key, val, _, to_end), part = partial_of(pair, early, late)
            at = slice(pair * LANES, (pair + 1) * LANES)
            tail = to_end[:, part]
            from_grad = state_part(v[:, at], swapped[pair])
            from_key = key_part(k[:, at].astype(F32) * tail, swapped[pair])
            writer.put(pair, key[:, part] + tail * from_grad, val[:, part] + from_key)
        writer.finish()

    @pl.when(jnp.logical_not(is_first))
    def _():
        writer = Writer(group, held, (rec_out,), sems)
        for pair in range(pairs):
            (rec, _, _, from_start, _), part = partial_of(pair, early, late)
            at = slice(pair * LANES, (pair + 1) * LANES)
            from_state = state_part(dy[:, at], swapped[pair])
            writer.put(pair, rec[:, part] + from_start[:, part] * from_state)
        writer.finish()


def share_kernel(blocks, sent, kept, got, mine, theirs):
    is_first = lax.axis_index("seq") == 0
    upper = lax.axis_index("dp") & 1
    last = sent.shape[0] - 1
    for b in range(blocks // 2):
        for ref, low in ((mine, upper), (theirs, 1 - upper)):
            p = 2 * b + low
            whole = jnp.where(is_first, sent[last, pl.ds(p, 1), :], got[last, pl.ds(p, 1), :])
            own, other = kept[p], got[p]
            ref[b] = jnp.where(is_first, own, other) + whole * jnp.where(is_first, other, own)


def halve_kernel(bit, mine, got, kept, theirs):
    upper = (lax.axis_index("dp") // bit) & 1
    for b in range(kept.shape[0]):
        for ref, low in ((kept, upper), (theirs, 1 - upper)):
            ref[b] = mine[2 * b + low] + got[2 * b + low]


def on_device(seq_size, dp_size, r, k, v, f, boost, dy, init):
    batch, toks, width = r.shape
    _, feature = boost.shape
    pairs = width // LANES
    group = 4 if pairs % 4 == 0 else 1
    state_group = 2 * group if pairs % (2 * group) == 0 else group
    half = feature // 2
    fast = (
        batch == 1
        and seq_size == 2
        and dp_size & (dp_size - 1) == 0
        and pairs == dp_size
        and pairs <= half
    )
    seq = lax.axis_index("seq")
    is_first = seq == 0
    init_t = init.T

    vmem = pl.BlockSpec(memory_space=pltpu.VMEM)
    anywhere = pl.BlockSpec(memory_space=pl.ANY)

    def limit(mib):
        return pltpu.CompilerParams(vmem_limit_bytes=mib * 2**20)

    def like(shape, kind=F32):
        return jax.ShapeDtypeStruct(shape, kind)

    def in_hbm(x):
        return pltpu.with_memory_space_constraint(x, pltpu.HBM)

    def states(b):
        if fast:
            shapes = (
                like((pairs + 1, half, LANES)),
                like((pairs, half, LANES)),
                like((pairs, feature, LANES)),
            )
        else:
            shapes = (
                like((pairs, feature, LANES)),
                like((pairs, feature, LANES)),
                like((pairs, 1, LANES)),
            )
        operands = (r[b], k[b], v[b], f[b], dy[b], init_t)
        outs = pl.pallas_call(
            lambda *refs: state_kernel(state_group, fast, *refs),
            in_specs=[anywhere] * 6,
            out_specs=(vmem,) * 9,
            out_shape=tuple(like(x.shape, x.dtype) for x in operands) + shapes,
            scratch_shapes=[pltpu.SemaphoreType.DMA((pairs // state_group, 6))],
            compiler_params=limit(24),
            name="states",
            cost_estimate=pl.CostEstimate(
                flops=4 * 10**9, bytes_accessed=4 * 2**20, transcendentals=10**6
            ),
        )(*(in_hbm(x) for x in operands))
        return outs[:6], outs[6:]

    def inner(near, first=0, count=pairs):
        def body(*refs):
            inner_kernel(first, count, UNROLL if count % UNROLL == 0 else 1, *refs)

        return pl.pallas_call(
            body,
            in_specs=[vmem] * 6,
            out_specs=(vmem,) * 5,
            out_shape=(like((toks, count * LANES)),) * 5,
            compiler_params=limit(24),
            name="inner",
            cost_estimate=pl.CostEstimate(
                flops=10**10, bytes_accessed=8 * 2**20, transcendentals=10**6
            ),
        )(*near[:5], boost)

    def outer(near, partial, start, after):
        rec, key, val, from_start, to_end = partial
        _, k, v, _, dy, _ = near
        here = pl.BlockSpec((toks, group * LANES), lambda i: (0, i))
        per_pair = pl.BlockSpec((group, feature, LANES), lambda i: (i, 0, 0))
        return pl.pallas_call(
            lambda *refs: outer_kernel(group, *refs),
            grid=(pairs // group,),
            in_specs=[here] * 8 + [per_pair] * 2,
            out_specs=(here,) * 3,
            out_shape=(like((toks, width), BF16),) * 3,
            compiler_params=limit(24),
            name="outer",
        )(k, v, dy, from_start, to_end, rec, key, val, start, after)

    def finish(kernel, operands, prior=()):
        count = len(operands)
        return pl.pallas_call(
            lambda *refs: kernel(group, *refs[:count], *refs[count + len(prior) :]),
            in_specs=[vmem] * count + [anywhere] * len(prior),
            out_specs=(anywhere,) * 3,
            out_shape=(like((toks, width), BF16),) * 3,
            scratch_shapes=[
                pltpu.VMEM((2, toks, width), BF16),
                pltpu.SemaphoreType.DMA((pairs // group, 2)),
            ],
            input_output_aliases={count + i: i for i in range(len(prior))},
            compiler_params=limit(24),
            cost_estimate=pl.CostEstimate(
                flops=3 * 10**9, bytes_accessed=9 * 2**20, transcendentals=0
            ),
        )(*operands, *prior)

    def share(sent, kept, got):
        shape = like((pairs // 2, half, LANES))
        return pl.pallas_call(
            lambda *refs: share_kernel(pairs, *refs),
            in_specs=[vmem] * 3,
            out_specs=(vmem,) * 2,
            out_shape=(shape,) * 2,
            compiler_params=limit(2),
            name="share",
        )(sent, kept, got)

    def halve(bit, mine, got):
        shape = like((mine.shape[0] // 2,) + mine.shape[1:])
        return pl.pallas_call(
            lambda *refs: halve_kernel(bit, *refs),
            in_specs=[vmem] * 2,
            out_specs=(vmem,) * 2,
            out_shape=(shape,) * 2,
            compiler_params=limit(2),
            name="halve",
        )(mine, got)

    if fast:
        near, (sent, kept, swapped) = states(0)
        swap = [(0, 1), (1, 0)]
        got = lax.ppermute(sent, "seq", swap)
        other = lax.ppermute(swapped, "seq", swap)
        cut = 3 * pairs // 4
        partial_a = inner(near, 0, cut)
        partial_b = inner(near, cut, pairs - cut)
        mine, theirs = share(sent, kept, got)
        bit = 1
        while True:
            got = lax.ppermute(theirs, "dp", [(i, i ^ bit) for i in range(dp_size)])
            bit *= 2
            if bit == dp_size:
                break
            mine, theirs = halve(bit, mine, got)
        total = mine + got
        state_grad = total.transpose(0, 2, 1).reshape(-1, half)
        _, k_near, v_near, _, dy_near, init_near = near
        partial = (*partial_a, *partial_b)
        results = finish(known_kernel, (dy_near, init_near, *partial))
        rec, key, val = finish(
            swapped_kernel, (k_near, v_near, dy_near, other, *partial), results
        )
        return rec[None], key[None], val[None], state_grad

    forward = [(i, i + 1) for i in range(seq_size - 1)]
    backward = [(i + 1, i) for i in range(seq_size - 1)]
    start_t = init_t.reshape(feature, pairs, LANES).transpose(1, 0, 2)
    results, term = [], 0.0
    for b in range(batch):
        near, (state_local, grad_local, whole) = states(b)
        start = start_t
        after = jnp.zeros_like(grad_local)
        for _ in range(seq_size - 1):
            end = whole * start + state_local
            start = jnp.where(is_first, start_t, lax.ppermute(end, "seq", forward))
            after = lax.ppermute(grad_local + whole * after, "seq", backward)
        results.append(outer(near, inner(near), start, after))
        term = term + jnp.where(is_first, grad_local + whole * after, 0.0)
    term = term.transpose(0, 2, 1).reshape(width, feature)
    summed = lax.psum_scatter(term, "dp", scatter_dimension=0, tiled=True)
    summed = lax.psum(summed, "seq")
    columns = feature // seq_size
    state_grad = lax.dynamic_slice_in_dim(summed, seq * columns, columns, 1)
    rec, key, val = (jnp.stack(x) for x in zip(*results))
    return rec, key, val, state_grad


def solution(mesh):
    sizes = dict(mesh.shape)
    rows = P("dp", "seq", None)

    def run(*args):
        return on_device(sizes["seq"], sizes["dp"], *args)

    return jax.shard_map(
        run,
        mesh=mesh,
        in_specs=(rows, rows, rows, rows, P(), rows, P()),
        out_specs=(rows, rows, rows, P("dp", "seq")),
        check_vma=False,
    )
```

```python
import jax
import jax.numpy as jnp
from jax import lax
from jax.experimental import pallas as pl
from jax.experimental.pallas import tpu as pltpu
from jax.sharding import PartitionSpec as P


LANES = 128
CHUNK = 32
UNROLL = 4
BF16 = jnp.bfloat16
F32 = jnp.float32


def dot(a, b, contract=(1, 0)):
    return lax.dot_general(
        a, b, (((contract[0],), (contract[1],)), ((), ())), preferred_element_type=F32
    )


def split(x):
    hi = x.astype(BF16)
    return hi, (x - hi.astype(F32)).astype(BF16)


def interleave(works):
    works = list(works)
    while works:
        works = [w for w in works if next(w, works) is not works]


def triangle(toks, after):
    row = lax.broadcasted_iota(jnp.int32, (toks, toks), 0)
    col = lax.broadcasted_iota(jnp.int32, (toks, toks), 1)
    same = (row // CHUNK) == (col // CHUNK)
    order = (col > row) if after else (col < row)
    return jnp.where(same & order, 1.0, 0.0).astype(BF16)


def log_sums(log_decay, *tris):
    hi, lo = split(log_decay)
    tri = jnp.concatenate(tris, 0)
    sums = dot(jnp.concatenate([tri, tri], 1), jnp.concatenate([hi, lo], 0))
    toks = log_decay.shape[0]
    return [sums[i * toks : (i + 1) * toks] for i in range(len(tris))]


def log_decay_of(fade):
    return -jnp.exp(fade.astype(F32))


def chunk_totals(sums, log_decay, after):
    totals = []
    for c in range(log_decay.shape[0] // CHUNK):
        at = c * CHUNK if after else (c + 1) * CHUNK - 1
        totals.append(sums[at : at + 1] + log_decay[at : at + 1])
    return totals


def spread(factors, totals, after):
    chunks = len(totals)
    order = range(chunks)[::-1] if after else range(chunks)
    pieces = [None] * chunks
    run = jnp.zeros_like(totals[0])
    for c in order:
        pieces[c] = factors[c * CHUNK : (c + 1) * CHUNK] * jnp.exp(run)
        run = run + totals[c]
    return jnp.concatenate(pieces, 0), jnp.exp(run)


def first_head(shape):
    return lax.broadcasted_iota(jnp.int32, shape, len(shape) - 1) < (LANES // 2)


def by_head(x):
    keep = first_head(x.shape)
    zero = jnp.zeros_like(x)
    return jnp.concatenate([jnp.where(keep, x, zero), jnp.where(keep, zero, x)], 0)


def diagonal(x):
    half = x.shape[0] // 2
    return jnp.where(first_head((half, LANES)), x[:half], x[half:])


def grad_kernel(group, fast, *refs):
    sources, refs = refs[:6], refs[6:]
    copies, refs = refs[:6], refs[6:]
    (from_out, *outs), sems = refs[:-1], refs[-1]
    f, r, dy = copies[:3]
    toks, width = r.shape
    steps = width // LANES // group
    is_first = lax.axis_index("seq") == 0

    def fetch(step, i):
        lanes = pl.ds(step * group * LANES, group * LANES)
        return pltpu.make_async_copy(
            sources[i].at[:, lanes], copies[i].at[:, lanes], sems.at[step, i]
        )

    for part in (range(3), range(3, 6)):
        for step in range(steps):
            for i in part:
                fetch(step, i).start()
    tri = triangle(toks, False)

    def work(pair):
        at = slice(pair * LANES, (pair + 1) * LANES)
        log_decay = log_decay_of(f[:, at])
        (before,) = log_sums(log_decay, tri)
        yield
        totals = chunk_totals(before, log_decay, False)
        from_start, whole = spread(jnp.exp(before), totals, False)
        from_out[:, at] = from_start
        rec_hi, rec_lo = split(r[:, at].astype(F32) * from_start)
        grad = dot(dy[:, at], jnp.concatenate([rec_hi, rec_lo], 1), (0, 0))
        yield
        grad = diagonal(grad[:, :LANES] + grad[:, LANES:])
        if fast:
            sent, kept = outs
            half = grad.shape[0] // 2
            sent[pair] = jnp.where(is_first, grad[half:], grad[:half])
            kept[pair] = jnp.where(is_first, grad[:half], grad[half:])
            sent[sent.shape[0] - 1, pair : pair + 1] = whole
        else:
            grads, wholes = outs
            grads[pair] = grad
            wholes[pair] = whole

    for step in range(steps):
        for i in range(3):
            fetch(step, i).wait()
        interleave(work(step * group + p) for p in range(group))
    for step in range(steps):
        for i in range(3, 6):
            fetch(step, i).wait()


def end_kernel(group, fast, f, k, v, init, *refs):
    to_out, state_out = refs[-2:]
    toks, width = k.shape
    tri = triangle(toks, True)
    is_first = lax.axis_index("seq") == 0

    def work(pair):
        at = slice(pair * LANES, (pair + 1) * LANES)
        log_decay = log_decay_of(f[:, at])
        (behind,) = log_sums(log_decay, tri)
        yield
        totals = chunk_totals(behind, log_decay, True)
        to_end, whole = spread(jnp.exp(behind), totals, True)
        to_out[:, at] = to_end
        key_hi, key_lo = split(k[:, at].astype(F32) * to_end)
        state = dot(v[:, at], jnp.concatenate([key_hi, key_lo], 1), (0, 0))
        yield
        state = diagonal(state[:, :LANES] + state[:, LANES:])
        if fast:
            sent, kept = refs[:2]
            grad = jnp.concatenate([sent[pair], kept[pair]], 0)
            state_out[pair] = jnp.where(is_first, whole * init[:, at] + state, grad)
        else:
            state_out[pair] = state

    for step in range(width // LANES // group):
        interleave(work(step * group + p) for p in range(group))


def inner_kernel(first, count, unroll, r, k, v, f, dy, boost, *outs):
    def step(i, carry):
        base = pl.multiple_of(i * unroll * LANES, LANES)
        inner_pairs(first * LANES + base, base, unroll, r, k, v, f, dy, boost, *outs)
        return carry

    lax.fori_loop(0, count // unroll, step, 0)


def inner_pairs(base, out_base, pairs, r, k, v, f, dy, boost, rec, key, val):
    toks = r.shape[0]
    chunks = toks // CHUNK
    tris = triangle(toks, False), triangle(toks, True)
    keep = first_head((toks, LANES))
    keep_chunk = first_head((CHUNK, LANES))
    row = lax.broadcasted_iota(jnp.int32, (CHUNK, CHUNK), 0)
    col = lax.broadcasted_iota(jnp.int32, (CHUNK, CHUNK), 1)
    wide_row = lax.broadcasted_iota(jnp.int32, (toks, toks), 0)
    wide_col = lax.broadcasted_iota(jnp.int32, (toks, toks), 1)
    below = wide_col < wide_row
    reversed_tok = (chunks - 1 - wide_col // CHUNK) * CHUNK + wide_col % CHUNK
    above = reversed_tok > wide_row

    def flip(x):
        return jnp.concatenate(
            [x[c * CHUNK : (c + 1) * CHUNK] for c in reversed(range(chunks))], 0
        )

    rows = [slice(c * CHUNK, (c + 1) * CHUNK) for c in range(chunks)]

    def work(p):
        at = pl.ds(pl.multiple_of(base + p * LANES, LANES), LANES)
        to = pl.ds(pl.multiple_of(out_base + p * LANES, LANES), LANES)
        log_decay = log_decay_of(f[:, at])
        before, behind = log_sums(log_decay, *tris)
        totals = chunk_totals(before, log_decay, False)
        mids = [c * CHUNK + CHUNK // 2 for c in range(chunks)]
        middles = [before[mid : mid + 1] for mid in mids]
        early, late = jnp.exp(before), jnp.exp(behind)
        rb, kb, vb, db = r[:, at], k[:, at], v[:, at], dy[:, at]
        rf, kf, vf, df = (x.astype(F32) for x in (rb, kb, vb, db))
        head = 2 * (base // LANES + p)
        u = jnp.concatenate([boost[pl.ds(head, 1)], boost[pl.ds(head + 1, 1)]], 1)
        rec_early = rf * early
        key_late = kf * late
        dy_heads = by_head(flip(db))
        scores = dot(db, by_head(vb), (1, 1))
        scores_split, scores_t_split = [], []
        for h in range(2):
            part = slice(h * toks, (h + 1) * toks)
            halves = split(jnp.where(below, scores[:, part], 0.0))
            scores_split.append(halves)
            scores_t_split.append([flip(x).T for x in halves])
        rec_rows, key_rows, cross_rows = [], [], []
        yield
        for c in range(chunks):
            here = rows[c]
            count = (c + 1) * CHUNK
            pieces = [key_late[here] * jnp.exp(middles[c] - totals[c])]
            gap = middles[c]
            for e in reversed(range(c)):
                pieces.append(key_late[rows[e]] * jnp.exp(gap))
                gap = gap + totals[e]
            key_hi, key_lo = split(jnp.concatenate(pieces[::-1], 0))
            stack = jnp.concatenate(
                [s[i][here, :count] for i in range(2) for s in scores_split], 0
            )
            got = dot(stack, jnp.concatenate([key_hi, key_lo], 1))
            got = got[:, :LANES] + got[:, LANES:]
            got = got[: 2 * CHUNK] + got[2 * CHUNK :]
            got = jnp.where(keep_chunk, got[:CHUNK], got[CHUNK:])
            rec_rows.append(early[here] * jnp.exp(-middles[c]) * got)
            pieces = [rec_early[here] * jnp.exp(-middles[c])]
            gap = totals[c] - middles[c]
            for e in range(c + 1, chunks):
                pieces.append(rec_early[rows[e]] * jnp.exp(gap))
                gap = gap + totals[e]
            rec_hi, rec_lo = split(jnp.concatenate(pieces[::-1], 0))
            count = (chunks - c) * CHUNK
            stack = jnp.concatenate(
                [s[i][here, :count] for i in range(2) for s in scores_t_split], 0
            )
            got = dot(stack, jnp.concatenate([rec_hi, rec_lo], 1))
            got = got[:, :LANES] + got[:, LANES:]
            got = got[: 2 * CHUNK] + got[2 * CHUNK :]
            got = jnp.where(keep_chunk, got[:CHUNK], got[CHUNK:])
            key_rows.append(late[here] * jnp.exp(middles[c] - totals[c]) * got)
            own = slice(c * CHUNK, (c + 1) * CHUNK)
            lhs = jnp.concatenate([by_head(key_hi[own]), by_head(key_lo[own])], 0)
            if c:
                pad = jnp.zeros((c * CHUNK, LANES), BF16)
                rhs = jnp.concatenate([rec_hi, pad, rec_lo, pad], 0)
            else:
                rhs = jnp.concatenate([rec_hi, rec_lo], 0)
            got = dot(lhs, rhs, (1, 1))
            got = got[:, :toks] + got[:, toks:]
            got = got[: 2 * CHUNK] + got[2 * CHUNK :]
            cross_rows.append(
                [jnp.where(above[here], got[h * CHUNK : (h + 1) * CHUNK], 0.0) for h in range(2)]
            )
            yield
        cross = jnp.concatenate(
            [jnp.concatenate([c[h] for c in cross_rows], 0) for h in range(2)], 1
        )
        cross_hi, cross_lo = split(cross)
        inner_val = dot(cross_hi, dy_heads) + dot(cross_lo, dy_heads)
        prod = vf * df
        mix = rf * u * kf

        def head_sum(x):
            one = jnp.sum(jnp.where(keep, x, 0.0), axis=-1, keepdims=True)
            two = jnp.sum(jnp.where(keep, 0.0, x), axis=-1, keepdims=True)
            return jnp.where(keep, one, two)

        boosted = u * head_sum(prod)
        rec[:, to] = jnp.concatenate(rec_rows, 0) + kf * boosted
        key[:, to] = jnp.concatenate(key_rows, 0) + rf * boosted
        val[:, to] = inner_val + head_sum(mix) * df

    interleave(work(p) for p in range(pairs))


def state_part(rows, state):
    hi, lo = split(by_head(state))
    return dot(jnp.concatenate([rows, rows], 1), jnp.concatenate([hi, lo], 0))


def key_part(keys, state):
    hi, lo = split(by_head(state))
    key_hi, key_lo = split(keys)
    wide = dot(key_hi, jnp.concatenate([hi, lo], 0), (1, 1))
    return wide[:, :LANES] + wide[:, LANES:] + dot(key_lo, hi, (1, 1))


def outer_kernel(pairs, k, v, dy, from_start, to_end, rec, key, val, start, after, *outs):
    rec_out, key_out, val_out = outs
    for p in range(pairs):
        at = slice(p * LANES, (p + 1) * LANES)
        tail = to_end[:, at]
        from_state = state_part(dy[:, at], start[p])
        rec_out[:, at] = (rec[:, at] + from_start[:, at] * from_state).astype(BF16)
        from_grad = state_part(v[:, at], after[p])
        key_out[:, at] = (key[:, at] + tail * from_grad).astype(BF16)
        from_key = key_part(k[:, at].astype(F32) * tail, after[p])
        val_out[:, at] = (val[:, at] + from_key).astype(BF16)


class Writer:
    def __init__(self, group, held, outs, sems):
        self.group, self.held, self.outs, self.sems = group, held, outs, sems
        self.started = []

    def put(self, pair, *values):
        at = slice(pair * LANES, (pair + 1) * LANES)
        for i, value in enumerate(values):
            self.held[i, :, at] = value.astype(BF16)
        if (pair + 1) % self.group == 0:
            step = pair // self.group
            lanes = pl.ds(step * self.group * LANES, self.group * LANES)
            for i in range(len(values)):
                copy = pltpu.make_async_copy(
                    self.held.at[i, :, lanes], self.outs[i].at[:, lanes], self.sems.at[step, i]
                )
                copy.start()
                self.started.append(copy)

    def finish(self):
        for copy in self.started:
            copy.wait()


def partial_of(pair, early, late):
    count = early[0].shape[1] // LANES
    refs, place = (early, pair) if pair < count else (late, pair - count)
    return refs, slice(place * LANES, (place + 1) * LANES)


def by_groups(group, pairs, work):
    for first in range(0, pairs, group):
        interleave(work(pair) for pair in range(first, first + group))


def rec_writer(group, dy, from_start, state_of, early, late, out, held, sems):
    writer = Writer(group, held, (out,), sems)

    def work(pair):
        rec, part = partial_of(pair, early, late)
        at = slice(pair * LANES, (pair + 1) * LANES)
        from_state = state_part(dy[:, at], state_of(pair))
        yield
        writer.put(pair, rec[0][:, part] + from_start[:, at] * from_state)

    by_groups(group, dy.shape[1] // LANES, work)
    writer.finish()


def known_kernel(group, dy, init, from_start, *refs):
    early, late, (rec_out, key_out, val_out, held, sems) = refs[:3], refs[3:6], refs[6:]
    is_first = lax.axis_index("seq") == 0

    @pl.when(is_first)
    def _():
        def state_of(pair):
            return init[:, pair * LANES : (pair + 1) * LANES]

        rec_writer(group, dy, from_start, state_of, early, late, rec_out, held, sems)

    @pl.when(jnp.logical_not(is_first))
    def _():
        writer = Writer(group, held, (key_out, val_out), sems)
        for pair in range(dy.shape[1] // LANES):
            (_, key, val), part = partial_of(pair, early, late)
            writer.put(pair, key[:, part], val[:, part])
        writer.finish()


def swapped_kernel(group, k, v, dy, swapped, from_start, to_end, *refs):
    early, late, outs = refs[:3], refs[3:6], refs[-5:]
    rec_out, key_out, val_out, held, sems = outs
    is_first = lax.axis_index("seq") == 0

    @pl.when(is_first)
    def _():
        writer = Writer(group, held, (key_out, val_out), sems)

        def work(pair):
            (_, key, val), part = partial_of(pair, early, late)
            at = slice(pair * LANES, (pair + 1) * LANES)
            tail = to_end[:, at]
            from_grad = state_part(v[:, at], swapped[pair])
            from_key = key_part(k[:, at].astype(F32) * tail, swapped[pair])
            yield
            writer.put(pair, key[:, part] + tail * from_grad, val[:, part] + from_key)

        by_groups(group, dy.shape[1] // LANES, work)
        writer.finish()

    @pl.when(jnp.logical_not(is_first))
    def _():
        def state_of(pair):
            return swapped[pair]

        rec_writer(group, dy, from_start, state_of, early, late, rec_out, held, sems)


def share_kernel(blocks, sent, kept, got, mine, theirs):
    is_first = lax.axis_index("seq") == 0
    upper = lax.axis_index("dp") & 1
    last = sent.shape[0] - 1
    for b in range(blocks // 2):
        for ref, low in ((mine, upper), (theirs, 1 - upper)):
            p = 2 * b + low
            whole = jnp.where(is_first, sent[last, pl.ds(p, 1), :], got[last, pl.ds(p, 1), :])
            own, other = kept[p], got[p]
            ref[b] = jnp.where(is_first, own, other) + whole * jnp.where(is_first, other, own)


def halve_kernel(bit, mine, got, kept, theirs):
    upper = (lax.axis_index("dp") // bit) & 1
    for b in range(kept.shape[0]):
        for ref, low in ((kept, upper), (theirs, 1 - upper)):
            ref[b] = mine[2 * b + low] + got[2 * b + low]


def on_device(seq_size, dp_size, r, k, v, f, boost, dy, init):
    batch, toks, width = r.shape
    _, feature = boost.shape
    pairs = width // LANES
    group = 4 if pairs % 4 == 0 else 1
    state_group = 2 * group if pairs % (2 * group) == 0 else group
    half = feature // 2
    fast = (
        batch == 1
        and seq_size == 2
        and dp_size & (dp_size - 1) == 0
        and pairs == dp_size
        and pairs <= half
    )
    seq = lax.axis_index("seq")
    is_first = seq == 0
    init_t = init.T

    vmem = pl.BlockSpec(memory_space=pltpu.VMEM)
    anywhere = pl.BlockSpec(memory_space=pl.ANY)

    def limit(mib):
        return pltpu.CompilerParams(vmem_limit_bytes=mib * 2**20)

    def like(shape, kind=F32):
        return jax.ShapeDtypeStruct(shape, kind)

    def in_hbm(x):
        return pltpu.with_memory_space_constraint(x, pltpu.HBM)

    def grads(b):
        if fast:
            shapes = (like((pairs + 1, half, LANES)), like((pairs, half, LANES)))
        else:
            shapes = (like((pairs, feature, LANES)), like((pairs, 1, LANES)))
        operands = (f[b], r[b], dy[b], k[b], v[b], init_t)
        outs = pl.pallas_call(
            lambda *refs: grad_kernel(state_group, fast, *refs),
            in_specs=[anywhere] * 6,
            out_specs=(vmem,) * (7 + len(shapes)),
            out_shape=tuple(like(x.shape, x.dtype) for x in operands)
            + (like((toks, width)),)
            + shapes,
            scratch_shapes=[pltpu.SemaphoreType.DMA((pairs // state_group, 6))],
            compiler_params=limit(24),
            name="grads",
            cost_estimate=pl.CostEstimate(
                flops=4 * 10**9, bytes_accessed=4 * 2**20, transcendentals=10**6
            ),
        )(*(in_hbm(x) for x in operands))
        return outs[:6], outs[6], outs[7:]

    def ends(near, *grad):
        f, _, _, k, v, init = near
        return pl.pallas_call(
            lambda *refs: end_kernel(state_group, fast, *refs),
            in_specs=[vmem] * (4 + len(grad)),
            out_specs=(vmem,) * 2,
            out_shape=(like((toks, width)), like((pairs, feature, LANES))),
            compiler_params=limit(24),
            name="ends",
            cost_estimate=pl.CostEstimate(
                flops=4 * 10**9, bytes_accessed=4 * 2**20, transcendentals=10**6
            ),
        )(f, k, v, init, *grad)

    def inner(near, first=0, count=pairs):
        def body(*refs):
            inner_kernel(first, count, UNROLL if count % UNROLL == 0 else 1, *refs)

        return pl.pallas_call(
            body,
            in_specs=[vmem] * 6,
            out_specs=(vmem,) * 3,
            out_shape=(like((toks, count * LANES)),) * 3,
            compiler_params=limit(24),
            name="inner",
            cost_estimate=pl.CostEstimate(
                flops=10**10, bytes_accessed=8 * 2**20, transcendentals=10**6
            ),
        )(near[1], near[3], near[4], near[0], near[2], boost)

    def outer(near, partial, from_start, to_end, start, after):
        rec, key, val = partial
        _, _, dy, k, v, _ = near
        here = pl.BlockSpec((toks, group * LANES), lambda i: (0, i))
        per_pair = pl.BlockSpec((group, feature, LANES), lambda i: (i, 0, 0))
        return pl.pallas_call(
            lambda *refs: outer_kernel(group, *refs),
            grid=(pairs // group,),
            in_specs=[here] * 8 + [per_pair] * 2,
            out_specs=(here,) * 3,
            out_shape=(like((toks, width), BF16),) * 3,
            compiler_params=limit(24),
            name="outer",
        )(k, v, dy, from_start, to_end, rec, key, val, start, after)

    def finish(kernel, operands, prior=()):
        count = len(operands)
        return pl.pallas_call(
            lambda *refs: kernel(group, *refs[:count], *refs[count + len(prior) :]),
            in_specs=[vmem] * count + [anywhere] * len(prior),
            out_specs=(anywhere,) * 3,
            out_shape=(like((toks, width), BF16),) * 3,
            scratch_shapes=[
                pltpu.VMEM((2, toks, width), BF16),
                pltpu.SemaphoreType.DMA((pairs // group, 2)),
            ],
            input_output_aliases={count + i: i for i in range(len(prior))},
            compiler_params=limit(24),
            cost_estimate=pl.CostEstimate(
                flops=3 * 10**9, bytes_accessed=9 * 2**20, transcendentals=0
            ),
        )(*operands, *prior)

    def share(sent, kept, got):
        shape = like((pairs // 2, half, LANES))
        return pl.pallas_call(
            lambda *refs: share_kernel(pairs, *refs),
            in_specs=[vmem] * 3,
            out_specs=(vmem,) * 2,
            out_shape=(shape,) * 2,
            compiler_params=limit(2),
            name="share",
        )(sent, kept, got)

    def halve(bit, mine, got):
        shape = like((mine.shape[0] // 2,) + mine.shape[1:])
        return pl.pallas_call(
            lambda *refs: halve_kernel(bit, *refs),
            in_specs=[vmem] * 2,
            out_specs=(vmem,) * 2,
            out_shape=(shape,) * 2,
            compiler_params=limit(2),
            name="halve",
        )(mine, got)

    if fast:
        near, from_start, (sent, kept) = grads(0)
        swap = [(0, 1), (1, 0)]
        got = lax.ppermute(sent, "seq", swap)
        to_end, swapped = ends(near, sent, kept)
        other = lax.ppermute(swapped, "seq", swap)
        cut = 3 * pairs // 4
        partial_a = inner(near, 0, cut)
        partial_b = inner(near, cut, pairs - cut)
        mine, theirs = share(sent, kept, got)
        bit = 1
        while True:
            got = lax.ppermute(theirs, "dp", [(i, i ^ bit) for i in range(dp_size)])
            bit *= 2
            if bit == dp_size:
                break
            mine, theirs = halve(bit, mine, got)
        total = mine + got
        state_grad = total.transpose(0, 2, 1).reshape(-1, half)
        _, _, dy_near, k_near, v_near, init_near = near
        partial = (*partial_a, *partial_b)
        results = finish(known_kernel, (dy_near, init_near, from_start, *partial))
        rec, key, val = finish(
            swapped_kernel,
            (k_near, v_near, dy_near, other, from_start, to_end, *partial),
            results,
        )
        return rec[None], key[None], val[None], state_grad

    forward = [(i, i + 1) for i in range(seq_size - 1)]
    backward = [(i + 1, i) for i in range(seq_size - 1)]
    start_t = init_t.reshape(feature, pairs, LANES).transpose(1, 0, 2)
    results, term = [], 0.0
    for b in range(batch):
        near, from_start, (grad_local, whole) = grads(b)
        to_end, state_local = ends(near)
        start = start_t
        after = jnp.zeros_like(grad_local)
        for _ in range(seq_size - 1):
            end = whole * start + state_local
            start = jnp.where(is_first, start_t, lax.ppermute(end, "seq", forward))
            after = lax.ppermute(grad_local + whole * after, "seq", backward)
        results.append(outer(near, inner(near), from_start, to_end, start, after))
        term = term + jnp.where(is_first, grad_local + whole * after, 0.0)
    term = term.transpose(0, 2, 1).reshape(width, feature)
    summed = lax.psum_scatter(term, "dp", scatter_dimension=0, tiled=True)
    summed = lax.psum(summed, "seq")
    columns = feature // seq_size
    state_grad = lax.dynamic_slice_in_dim(summed, seq * columns, columns, 1)
    rec, key, val = (jnp.stack(x) for x in zip(*results))
    return rec, key, val, state_grad


def solution(mesh):
    sizes = dict(mesh.shape)
    rows = P("dp", "seq", None)

    def run(*args):
        return on_device(sizes["seq"], sizes["dp"], *args)

    return jax.shard_map(
        run,
        mesh=mesh,
        in_specs=(rows, rows, rows, rows, P(), rows, P()),
        out_specs=(rows, rows, rows, P("dp", "seq")),
        check_vma=False,
    )
```

```python
import jax
import jax.numpy as jnp
from jax import lax
from jax.experimental import pallas as pl
from jax.experimental.pallas import tpu as pltpu
from jax.sharding import PartitionSpec as P


LANES = 128
CHUNK = 32
UNROLL = 4
BF16 = jnp.bfloat16
F32 = jnp.float32


def dot(a, b, contract=(1, 0)):
    return lax.dot_general(
        a, b, (((contract[0],), (contract[1],)), ((), ())), preferred_element_type=F32
    )


def split(x):
    hi = x.astype(BF16)
    return hi, (x - hi.astype(F32)).astype(BF16)


def interleave(works):
    works = list(works)
    while works:
        works = [w for w in works if next(w, works) is not works]


def triangle(toks, after):
    row = lax.broadcasted_iota(jnp.int32, (toks, toks), 0)
    col = lax.broadcasted_iota(jnp.int32, (toks, toks), 1)
    same = (row // CHUNK) == (col // CHUNK)
    order = (col > row) if after else (col < row)
    return jnp.where(same & order, 1.0, 0.0).astype(BF16)


def log_sums(log_decay, *tris):
    hi, lo = split(log_decay)
    tri = jnp.concatenate(tris, 0)
    sums = dot(jnp.concatenate([tri, tri], 1), jnp.concatenate([hi, lo], 0))
    toks = log_decay.shape[0]
    return [sums[i * toks : (i + 1) * toks] for i in range(len(tris))]


def log_decay_of(fade):
    return -jnp.exp(fade.astype(F32))


def chunk_totals(sums, log_decay, after):
    totals = []
    for c in range(log_decay.shape[0] // CHUNK):
        at = c * CHUNK if after else (c + 1) * CHUNK - 1
        totals.append(sums[at : at + 1] + log_decay[at : at + 1])
    return totals


def spread(factors, totals, after):
    chunks = len(totals)
    order = range(chunks)[::-1] if after else range(chunks)
    pieces = [None] * chunks
    run = jnp.zeros_like(totals[0])
    for c in order:
        pieces[c] = factors[c * CHUNK : (c + 1) * CHUNK] * jnp.exp(run)
        run = run + totals[c]
    return jnp.concatenate(pieces, 0), jnp.exp(run)


def first_head(shape):
    return lax.broadcasted_iota(jnp.int32, shape, len(shape) - 1) < (LANES // 2)


def by_head(x):
    keep = first_head(x.shape)
    zero = jnp.zeros_like(x)
    return jnp.concatenate([jnp.where(keep, x, zero), jnp.where(keep, zero, x)], 0)


def diagonal(x):
    half = x.shape[0] // 2
    return jnp.where(first_head((half, LANES)), x[:half], x[half:])


def grad_kernel(group, fast, *refs):
    sources, refs = refs[:6], refs[6:]
    copies, refs = refs[:6], refs[6:]
    (from_out, *outs), sems = refs[:-1], refs[-1]
    f, r, dy = copies[:3]
    toks, width = r.shape
    steps = width // LANES // group
    is_first = lax.axis_index("seq") == 0

    def fetch(step, i):
        lanes = pl.ds(step * group * LANES, group * LANES)
        return pltpu.make_async_copy(
            sources[i].at[:, lanes], copies[i].at[:, lanes], sems.at[step, i]
        )

    for part in (range(3), range(3, 6)):
        for step in range(steps):
            for i in part:
                fetch(step, i).start()
    tri = triangle(toks, False)

    def work(pair):
        at = slice(pair * LANES, (pair + 1) * LANES)
        log_decay = log_decay_of(f[:, at])
        (before,) = log_sums(log_decay, tri)
        yield
        totals = chunk_totals(before, log_decay, False)
        from_start, whole = spread(jnp.exp(before), totals, False)
        from_out[:, at] = from_start
        rec_hi, rec_lo = split(r[:, at].astype(F32) * from_start)
        grad = dot(dy[:, at], jnp.concatenate([rec_hi, rec_lo], 1), (0, 0))
        yield
        grad = diagonal(grad[:, :LANES] + grad[:, LANES:])
        if fast:
            sent, kept = outs
            half = grad.shape[0] // 2
            sent[pair * half : (pair + 1) * half] = jnp.where(is_first, grad[half:], grad[:half])
            kept[pair] = jnp.where(is_first, grad[:half], grad[half:])
            row = kept.shape[0] * half + pair
            sent[row : row + 1] = whole
        else:
            grads, wholes = outs
            grads[pair] = grad
            wholes[pair] = whole

    for step in range(steps):
        for i in range(3):
            fetch(step, i).wait()
        interleave(work(step * group + p) for p in range(group))
    for step in range(steps):
        for i in range(3, 6):
            fetch(step, i).wait()


def end_kernel(group, fast, f, k, v, init, *refs):
    to_out, state_out = refs[-2:]
    toks, width = k.shape
    tri = triangle(toks, True)
    is_first = lax.axis_index("seq") == 0

    def work(pair):
        at = slice(pair * LANES, (pair + 1) * LANES)
        log_decay = log_decay_of(f[:, at])
        (behind,) = log_sums(log_decay, tri)
        yield
        totals = chunk_totals(behind, log_decay, True)
        to_end, whole = spread(jnp.exp(behind), totals, True)
        to_out[:, at] = to_end
        key_hi, key_lo = split(k[:, at].astype(F32) * to_end)
        state = dot(v[:, at], jnp.concatenate([key_hi, key_lo], 1), (0, 0))
        yield
        state = diagonal(state[:, :LANES] + state[:, LANES:])
        if fast:
            sent, kept = refs[:2]
            half = kept.shape[1]
            grad = jnp.concatenate([sent[pair * half : (pair + 1) * half], kept[pair]], 0)
            state_out[pair] = jnp.where(is_first, whole * init[:, at] + state, grad)
        else:
            state_out[pair] = state

    for step in range(width // LANES // group):
        interleave(work(step * group + p) for p in range(group))


def inner_kernel(first, count, unroll, r, k, v, f, dy, boost, *outs):
    def step(i, carry):
        base = pl.multiple_of(i * unroll * LANES, LANES)
        inner_pairs(first * LANES + base, base, unroll, r, k, v, f, dy, boost, *outs)
        return carry

    lax.fori_loop(0, count // unroll, step, 0)


def inner_pairs(base, out_base, pairs, r, k, v, f, dy, boost, rec, key, val):
    toks = r.shape[0]
    chunks = toks // CHUNK
    tris = triangle(toks, False), triangle(toks, True)
    keep = first_head((toks, LANES))
    keep_chunk = first_head((CHUNK, LANES))
    row = lax.broadcasted_iota(jnp.int32, (CHUNK, CHUNK), 0)
    col = lax.broadcasted_iota(jnp.int32, (CHUNK, CHUNK), 1)
    wide_row = lax.broadcasted_iota(jnp.int32, (toks, toks), 0)
    wide_col = lax.broadcasted_iota(jnp.int32, (toks, toks), 1)
    below = wide_col < wide_row
    reversed_tok = (chunks - 1 - wide_col // CHUNK) * CHUNK + wide_col % CHUNK
    above = reversed_tok > wide_row

    def flip(x):
        return jnp.concatenate(
            [x[c * CHUNK : (c + 1) * CHUNK] for c in reversed(range(chunks))], 0
        )

    rows = [slice(c * CHUNK, (c + 1) * CHUNK) for c in range(chunks)]

    def work(p):
        at = pl.ds(pl.multiple_of(base + p * LANES, LANES), LANES)
        to = pl.ds(pl.multiple_of(out_base + p * LANES, LANES), LANES)
        log_decay = log_decay_of(f[:, at])
        before, behind = log_sums(log_decay, *tris)
        totals = chunk_totals(before, log_decay, False)
        mids = [c * CHUNK + CHUNK // 2 for c in range(chunks)]
        middles = [before[mid : mid + 1] for mid in mids]
        early, late = jnp.exp(before), jnp.exp(behind)
        rb, kb, vb, db = r[:, at], k[:, at], v[:, at], dy[:, at]
        rf, kf, vf, df = (x.astype(F32) for x in (rb, kb, vb, db))
        head = 2 * (base // LANES + p)
        u = jnp.concatenate([boost[pl.ds(head, 1)], boost[pl.ds(head + 1, 1)]], 1)
        rec_early = rf * early
        key_late = kf * late
        dy_heads = by_head(flip(db))
        scores = dot(db, by_head(vb), (1, 1))
        scores_split, scores_t_split = [], []
        for h in range(2):
            part = slice(h * toks, (h + 1) * toks)
            halves = split(jnp.where(below, scores[:, part], 0.0))
            scores_split.append(halves)
            scores_t_split.append([flip(x).T for x in halves])
        rec_rows, key_rows, cross_rows = [], [], []
        yield
        for c in range(chunks):
            here = rows[c]
            count = (c + 1) * CHUNK
            pieces = [kf[here] * (late[here] * jnp.exp(middles[c] - totals[c]))]
            gap = middles[c]
            for e in reversed(range(c)):
                pieces.append(key_late[rows[e]] * jnp.exp(gap))
                gap = gap + totals[e]
            key_hi, key_lo = split(jnp.concatenate(pieces[::-1], 0))
            stack = jnp.concatenate(
                [s[i][here, :count] for i in range(2) for s in scores_split], 0
            )
            got = dot(stack, jnp.concatenate([key_hi, key_lo], 1))
            got = got[:, :LANES] + got[:, LANES:]
            got = got[: 2 * CHUNK] + got[2 * CHUNK :]
            got = jnp.where(keep_chunk, got[:CHUNK], got[CHUNK:])
            rec_rows.append(early[here] * jnp.exp(-middles[c]) * got)
            pieces = [rf[here] * (early[here] * jnp.exp(-middles[c]))]
            gap = totals[c] - middles[c]
            for e in range(c + 1, chunks):
                pieces.append(rec_early[rows[e]] * jnp.exp(gap))
                gap = gap + totals[e]
            rec_hi, rec_lo = split(jnp.concatenate(pieces[::-1], 0))
            count = (chunks - c) * CHUNK
            stack = jnp.concatenate(
                [s[i][here, :count] for i in range(2) for s in scores_t_split], 0
            )
            got = dot(stack, jnp.concatenate([rec_hi, rec_lo], 1))
            got = got[:, :LANES] + got[:, LANES:]
            got = got[: 2 * CHUNK] + got[2 * CHUNK :]
            got = jnp.where(keep_chunk, got[:CHUNK], got[CHUNK:])
            key_rows.append(late[here] * jnp.exp(middles[c] - totals[c]) * got)
            own = slice(c * CHUNK, (c + 1) * CHUNK)
            lhs = jnp.concatenate([by_head(key_hi[own]), by_head(key_lo[own])], 0)
            if c:
                pad = jnp.zeros((c * CHUNK, LANES), BF16)
                rhs = jnp.concatenate([rec_hi, pad, rec_lo, pad], 0)
            else:
                rhs = jnp.concatenate([rec_hi, rec_lo], 0)
            got = dot(lhs, rhs, (1, 1))
            got = got[:, :toks] + got[:, toks:]
            got = got[: 2 * CHUNK] + got[2 * CHUNK :]
            cross_rows.append(
                [jnp.where(above[here], got[h * CHUNK : (h + 1) * CHUNK], 0.0) for h in range(2)]
            )
            yield
        cross = jnp.concatenate(
            [jnp.concatenate([c[h] for c in cross_rows], 0) for h in range(2)], 1
        )
        cross_hi, cross_lo = split(cross)
        inner_val = dot(cross_hi, dy_heads) + dot(cross_lo, dy_heads)
        prod = vf * df
        mix = rf * u * kf

        def head_sum(x):
            one = jnp.sum(jnp.where(keep, x, 0.0), axis=-1, keepdims=True)
            two = jnp.sum(jnp.where(keep, 0.0, x), axis=-1, keepdims=True)
            return jnp.where(keep, one, two)

        boosted = u * head_sum(prod)
        rec[:, to] = jnp.concatenate(rec_rows, 0) + kf * boosted
        key[:, to] = jnp.concatenate(key_rows, 0) + rf * boosted
        val[:, to] = inner_val + head_sum(mix) * df

    interleave(work(p) for p in range(pairs))


def state_part(rows, state):
    hi, lo = split(by_head(state))
    return dot(jnp.concatenate([rows, rows], 1), jnp.concatenate([hi, lo], 0))


def key_part(keys, state):
    hi, lo = split(by_head(state))
    key_hi, key_lo = split(keys)
    wide = dot(key_hi, jnp.concatenate([hi, lo], 0), (1, 1))
    return wide[:, :LANES] + wide[:, LANES:] + dot(key_lo, hi, (1, 1))


def outer_kernel(pairs, k, v, dy, from_start, to_end, rec, key, val, start, after, *outs):
    rec_out, key_out, val_out = outs
    for p in range(pairs):
        at = slice(p * LANES, (p + 1) * LANES)
        tail = to_end[:, at]
        from_state = state_part(dy[:, at], start[p])
        rec_out[:, at] = (rec[:, at] + from_start[:, at] * from_state).astype(BF16)
        from_grad = state_part(v[:, at], after[p])
        key_out[:, at] = (key[:, at] + tail * from_grad).astype(BF16)
        from_key = key_part(k[:, at].astype(F32) * tail, after[p])
        val_out[:, at] = (val[:, at] + from_key).astype(BF16)


class Writer:
    def __init__(self, group, held, outs, sems):
        self.group, self.held, self.outs, self.sems = group, held, outs, sems
        self.started = []

    def put(self, pair, *values):
        at = slice(pair * LANES, (pair + 1) * LANES)
        for i, value in enumerate(values):
            self.held[i, :, at] = value.astype(BF16)
        if (pair + 1) % self.group == 0:
            step = pair // self.group
            lanes = pl.ds(step * self.group * LANES, self.group * LANES)
            for i in range(len(values)):
                copy = pltpu.make_async_copy(
                    self.held.at[i, :, lanes], self.outs[i].at[:, lanes], self.sems.at[step, i]
                )
                copy.start()
                self.started.append(copy)

    def finish(self):
        for copy in self.started:
            copy.wait()


def partial_of(pair, early, late):
    count = early[0].shape[1] // LANES
    refs, place = (early, pair) if pair < count else (late, pair - count)
    return refs, slice(place * LANES, (place + 1) * LANES)


def by_groups(group, pairs, work):
    for first in range(0, pairs, group):
        interleave(work(pair) for pair in range(first, first + group))


def rec_writer(group, dy, from_start, state_of, early, late, out, held, sems):
    writer = Writer(group, held, (out,), sems)

    def work(pair):
        rec, part = partial_of(pair, early, late)
        at = slice(pair * LANES, (pair + 1) * LANES)
        from_state = state_part(dy[:, at], state_of(pair))
        yield
        writer.put(pair, rec[0][:, part] + from_start[:, at] * from_state)

    by_groups(group, dy.shape[1] // LANES, work)
    writer.finish()


def known_kernel(group, dy, init, from_start, *refs):
    early, late, (rec_out, key_out, val_out, held, sems) = refs[:3], refs[3:6], refs[6:]
    is_first = lax.axis_index("seq") == 0

    @pl.when(is_first)
    def _():
        def state_of(pair):
            return init[:, pair * LANES : (pair + 1) * LANES]

        rec_writer(group, dy, from_start, state_of, early, late, rec_out, held, sems)

    @pl.when(jnp.logical_not(is_first))
    def _():
        writer = Writer(group, held, (key_out, val_out), sems)
        for pair in range(dy.shape[1] // LANES):
            (_, key, val), part = partial_of(pair, early, late)
            writer.put(pair, key[:, part], val[:, part])
        writer.finish()


def swapped_kernel(group, k, v, dy, swapped, from_start, to_end, *refs):
    early, late, outs = refs[:3], refs[3:6], refs[-5:]
    rec_out, key_out, val_out, held, sems = outs
    is_first = lax.axis_index("seq") == 0

    @pl.when(is_first)
    def _():
        writer = Writer(group, held, (key_out, val_out), sems)

        def work(pair):
            (_, key, val), part = partial_of(pair, early, late)
            at = slice(pair * LANES, (pair + 1) * LANES)
            tail = to_end[:, at]
            from_grad = state_part(v[:, at], swapped[pair])
            from_key = key_part(k[:, at].astype(F32) * tail, swapped[pair])
            yield
            writer.put(pair, key[:, part] + tail * from_grad, val[:, part] + from_key)

        by_groups(group, dy.shape[1] // LANES, work)
        writer.finish()

    @pl.when(jnp.logical_not(is_first))
    def _():
        def state_of(pair):
            return swapped[pair]

        rec_writer(group, dy, from_start, state_of, early, late, rec_out, held, sems)


def share_kernel(blocks, sent, kept, got, mine, theirs):
    is_first = lax.axis_index("seq") == 0
    upper = lax.axis_index("dp") & 1
    half = kept.shape[1]
    for b in range(blocks // 2):
        for ref, low in ((mine, upper), (theirs, 1 - upper)):
            p = 2 * b + low
            row = pl.ds(blocks * half + p, 1)
            whole = jnp.where(is_first, sent[row], got[row])
            own, other = kept[p], got[pl.ds(pl.multiple_of(p * half, half), half)]
            ref[b] = jnp.where(is_first, own, other) + whole * jnp.where(is_first, other, own)


def halve_kernel(bit, mine, got, kept, theirs):
    upper = (lax.axis_index("dp") // bit) & 1
    for b in range(kept.shape[0]):
        for ref, low in ((kept, upper), (theirs, 1 - upper)):
            ref[b] = mine[2 * b + low] + got[2 * b + low]


def on_device(seq_size, dp_size, r, k, v, f, boost, dy, init):
    batch, toks, width = r.shape
    _, feature = boost.shape
    pairs = width // LANES
    group = 4 if pairs % 4 == 0 else 1
    state_group = 2 * group if pairs % (2 * group) == 0 else group
    half = feature // 2
    fast = (
        batch == 1
        and seq_size == 2
        and dp_size & (dp_size - 1) == 0
        and pairs == dp_size
        and pairs % 8 == 0
    )
    seq = lax.axis_index("seq")
    is_first = seq == 0
    init_t = init.T

    vmem = pl.BlockSpec(memory_space=pltpu.VMEM)
    anywhere = pl.BlockSpec(memory_space=pl.ANY)

    def limit(mib):
        return pltpu.CompilerParams(vmem_limit_bytes=mib * 2**20)

    def like(shape, kind=F32):
        return jax.ShapeDtypeStruct(shape, kind)

    def in_hbm(x):
        return pltpu.with_memory_space_constraint(x, pltpu.HBM)

    def grads(b):
        if fast:
            shapes = (like((pairs * (half + 1), LANES)), like((pairs, half, LANES)))
        else:
            shapes = (like((pairs, feature, LANES)), like((pairs, 1, LANES)))
        operands = (f[b], r[b], dy[b], k[b], v[b], init_t)
        outs = pl.pallas_call(
            lambda *refs: grad_kernel(state_group, fast, *refs),
            in_specs=[anywhere] * 6,
            out_specs=(vmem,) * (7 + len(shapes)),
            out_shape=tuple(like(x.shape, x.dtype) for x in operands)
            + (like((toks, width)),)
            + shapes,
            scratch_shapes=[pltpu.SemaphoreType.DMA((pairs // state_group, 6))],
            compiler_params=limit(24),
            name="grads",
            cost_estimate=pl.CostEstimate(
                flops=4 * 10**9, bytes_accessed=4 * 2**20, transcendentals=10**6
            ),
        )(*(in_hbm(x) for x in operands))
        return outs[:6], outs[6], outs[7:]

    def ends(near, *grad):
        f, _, _, k, v, init = near
        return pl.pallas_call(
            lambda *refs: end_kernel(state_group, fast, *refs),
            in_specs=[vmem] * (4 + len(grad)),
            out_specs=(vmem,) * 2,
            out_shape=(like((toks, width)), like((pairs, feature, LANES))),
            compiler_params=limit(24),
            name="ends",
            cost_estimate=pl.CostEstimate(
                flops=4 * 10**9, bytes_accessed=4 * 2**20, transcendentals=10**6
            ),
        )(f, k, v, init, *grad)

    def inner(near, first=0, count=pairs):
        def body(*refs):
            inner_kernel(first, count, UNROLL if count % UNROLL == 0 else 1, *refs)

        return pl.pallas_call(
            body,
            in_specs=[vmem] * 6,
            out_specs=(vmem,) * 3,
            out_shape=(like((toks, count * LANES)),) * 3,
            compiler_params=limit(24),
            name="inner",
            cost_estimate=pl.CostEstimate(
                flops=10**10, bytes_accessed=8 * 2**20, transcendentals=10**6
            ),
        )(near[1], near[3], near[4], near[0], near[2], boost)

    def outer(near, partial, from_start, to_end, start, after):
        rec, key, val = partial
        _, _, dy, k, v, _ = near
        here = pl.BlockSpec((toks, group * LANES), lambda i: (0, i))
        per_pair = pl.BlockSpec((group, feature, LANES), lambda i: (i, 0, 0))
        return pl.pallas_call(
            lambda *refs: outer_kernel(group, *refs),
            grid=(pairs // group,),
            in_specs=[here] * 8 + [per_pair] * 2,
            out_specs=(here,) * 3,
            out_shape=(like((toks, width), BF16),) * 3,
            compiler_params=limit(24),
            name="outer",
        )(k, v, dy, from_start, to_end, rec, key, val, start, after)

    def finish(kernel, operands, prior=()):
        count = len(operands)
        return pl.pallas_call(
            lambda *refs: kernel(group, *refs[:count], *refs[count + len(prior) :]),
            in_specs=[vmem] * count + [anywhere] * len(prior),
            out_specs=(anywhere,) * 3,
            out_shape=(like((toks, width), BF16),) * 3,
            scratch_shapes=[
                pltpu.VMEM((2, toks, width), BF16),
                pltpu.SemaphoreType.DMA((pairs // group, 2)),
            ],
            input_output_aliases={count + i: i for i in range(len(prior))},
            compiler_params=limit(24),
            cost_estimate=pl.CostEstimate(
                flops=3 * 10**9, bytes_accessed=9 * 2**20, transcendentals=0
            ),
        )(*operands, *prior)

    def share(sent, kept, got):
        shape = like((pairs // 2, half, LANES))
        return pl.pallas_call(
            lambda *refs: share_kernel(pairs, *refs),
            in_specs=[vmem] * 3,
            out_specs=(vmem,) * 2,
            out_shape=(shape,) * 2,
            compiler_params=limit(2),
            name="share",
        )(sent, kept, got)

    def halve(bit, mine, got):
        shape = like((mine.shape[0] // 2,) + mine.shape[1:])
        return pl.pallas_call(
            lambda *refs: halve_kernel(bit, *refs),
            in_specs=[vmem] * 2,
            out_specs=(vmem,) * 2,
            out_shape=(shape,) * 2,
            compiler_params=limit(2),
            name="halve",
        )(mine, got)

    if fast:
        near, from_start, (sent, kept) = grads(0)
        swap = [(0, 1), (1, 0)]
        got = lax.ppermute(sent, "seq", swap)
        to_end, swapped = ends(near, sent, kept)
        other = lax.ppermute(swapped, "seq", swap)
        cut = 3 * pairs // 4
        partial_a = inner(near, 0, cut)
        partial_b = inner(near, cut, pairs - cut)
        mine, theirs = share(sent, kept, got)
        bit = 1
        while True:
            got = lax.ppermute(theirs, "dp", [(i, i ^ bit) for i in range(dp_size)])
            bit *= 2
            if bit == dp_size:
                break
            mine, theirs = halve(bit, mine, got)
        total = mine + got
        state_grad = total.transpose(0, 2, 1).reshape(-1, half)
        _, _, dy_near, k_near, v_near, init_near = near
        partial = (*partial_a, *partial_b)
        results = finish(known_kernel, (dy_near, init_near, from_start, *partial))
        rec, key, val = finish(
            swapped_kernel,
            (k_near, v_near, dy_near, other, from_start, to_end, *partial),
            results,
        )
        return rec[None], key[None], val[None], state_grad

    forward = [(i, i + 1) for i in range(seq_size - 1)]
    backward = [(i + 1, i) for i in range(seq_size - 1)]
    start_t = init_t.reshape(feature, pairs, LANES).transpose(1, 0, 2)
    results, term = [], 0.0
    for b in range(batch):
        near, from_start, (grad_local, whole) = grads(b)
        to_end, state_local = ends(near)
        start = start_t
        after = jnp.zeros_like(grad_local)
        for _ in range(seq_size - 1):
            end = whole * start + state_local
            start = jnp.where(is_first, start_t, lax.ppermute(end, "seq", forward))
            after = lax.ppermute(grad_local + whole * after, "seq", backward)
        results.append(outer(near, inner(near), from_start, to_end, start, after))
        term = term + jnp.where(is_first, grad_local + whole * after, 0.0)
    term = term.transpose(0, 2, 1).reshape(width, feature)
    summed = lax.psum_scatter(term, "dp", scatter_dimension=0, tiled=True)
    summed = lax.psum(summed, "seq")
    columns = feature // seq_size
    state_grad = lax.dynamic_slice_in_dim(summed, seq * columns, columns, 1)
    rec, key, val = (jnp.stack(x) for x in zip(*results))
    return rec, key, val, state_grad


def solution(mesh):
    sizes = dict(mesh.shape)
    rows = P("dp", "seq", None)

    def run(*args):
        return on_device(sizes["seq"], sizes["dp"], *args)

    return jax.shard_map(
        run,
        mesh=mesh,
        in_specs=(rows, rows, rows, rows, P(), rows, P()),
        out_specs=(rows, rows, rows, P("dp", "seq")),
        check_vma=False,
    )
```
